32 devices in a mesh: gz: 2 (over x), gx: 4 (over y, core), gy: 4 (over z).
Axes of the slice: x: 2, y: 2, z: 4, core: 2. Of those that a mesh axis runs over, the one named last changes fastest.
Arguments:
- right_side: float32 [16, 3, 32, 1024], P('gz', None, 'gy', 'gx'), may hold values from -6 to 6
- start_field: float32 [16, 3, 32, 1024], P('gz', None, 'gy', 'gx'), may hold values from -6 to 6
- layer_material: int32 [16], P('gz'), may hold values from 0 to 7
- stiffness: float32 [8, 3, 3, 3], replicated, may hold values from -0.2 to 8, as said below
- line_factors: float32 [8, 3, 3, 3], replicated, may hold values from -0.05 to 1
Outputs:
- solution_field: float32 [16, 3, 32, 1024], P('gz', None, 'gy', 'gx')
- final_residual: float32 [16, 3, 32, 1024], P('gz', None, 'gy', 'gx')
The draws below stay inside these ranges and needn't reach their ends.
Inputs may be any that keep to these rules, and one draw needn't show every extreme that they name: `stiffness`: diagonal blocks dominate each row over the lateral and vertical couplings of the stencil.
All inputs are finite; a program needn't handle non-finite values.
Results may differ from the reference program's by a relative error of at most 0.0001.
Values sent between devices are 32-bit elements; how exact they have to be, the bound alone decides.
A program may use at most 64 MiB of HBM per device.

```python
import jax
import jax.numpy as jnp
from jax import lax

MATS = 8
SWEEPS = 3
NZ = 16
NY = 32
NX = 1024


def symmetric_noise(key, scale):
    noise = jax.random.uniform(key, (MATS, 3, 3), jnp.float32, -1.0, 1.0)
    both = 0.5 * (noise + jnp.swapaxes(noise, 1, 2))
    return scale * both * (1.0 - jnp.eye(3, dtype=jnp.float32))


def draw_stiffness(key, part):
    keys = jax.random.split(jax.random.fold_in(key, 11), 6)
    eye = jnp.eye(3, dtype=jnp.float32)
    lateral_rate = jax.random.uniform(keys[0], (MATS, 3), jnp.float32, 0.1, 0.3)
    vertical_rate = jax.random.uniform(keys[1], (MATS, 3), jnp.float32, 0.5, 1.5)
    margin = jax.random.uniform(keys[2], (MATS, 3), jnp.float32, 0.3, 1.0)
    lateral_off = symmetric_noise(keys[3], 0.03)
    vertical_off = symmetric_noise(keys[4], 0.1)
    diagonal_off = symmetric_noise(keys[5], 0.2)
    lateral_block = eye * lateral_rate[:, :, None] + lateral_off
    vertical_block = eye * vertical_rate[:, :, None] + vertical_off
    diagonal_value = 4.0 * lateral_rate + 2.0 * vertical_rate + margin
    diagonal_value = diagonal_value + 4.0 * jnp.sum(jnp.abs(lateral_off), axis=2)
    diagonal_value = diagonal_value + 2.0 * jnp.sum(jnp.abs(vertical_off), axis=2)
    diagonal_value = diagonal_value + jnp.sum(jnp.abs(diagonal_off), axis=2)
    diagonal_block = eye * diagonal_value[:, :, None] + diagonal_off
    return jnp.stack([diagonal_block, lateral_block, vertical_block], axis=1)


def draw_line_factors(key, part):
    keys = jax.random.split(jax.random.fold_in(key, 23), 8)
    eye = jnp.eye(3, dtype=jnp.float32)
    fast_comp = jax.random.randint(keys[0], (), 0, 3)
    quick_mask = jnp.arange(3)[None, :] == fast_comp

    def rates(first_key, second_key):
        slow = 1.0 - jnp.exp(jax.random.uniform(first_key, (MATS, 3), jnp.float32, jnp.log(1.0 / NZ), jnp.log(3.0 / NZ)))
        quick = 1.0 - jax.random.uniform(second_key, (MATS, 3), jnp.float32, 0.03, 0.08)
        return jnp.where(quick_mask, quick, slow)
    forward_rate = rates(keys[1], keys[2])
    backward_rate = rates(keys[3], keys[4])

    def multiplier(rate, sub_key):
        root = jnp.sqrt(1.0 - rate)
        coupling = 0.1 * root[:, :, None] * symmetric_noise(sub_key, 1.0) * root[:, None, :]
        return eye * rate[:, :, None] + coupling
    forward_block = multiplier(forward_rate, keys[5])
    backward_block = multiplier(backward_rate, keys[6])
    gain = 1.5 * (1.0 - forward_rate) * (1.0 - backward_rate)
    pivot_block = gain[:, :, None] * (eye + symmetric_noise(keys[7], 0.1))
    return jnp.stack([pivot_block, forward_block, backward_block], axis=1)


def touch_ends(values, stream_key, smallest, high):
    longest = values.shape.index(max(values.shape))
    spots = []
    for shift in (0, 1):
        where = [jax.random.randint(jax.random.fold_in(stream_key, axis), (), 0, length) for axis, length in enumerate(values.shape)]
        where[longest] = (where[longest] + shift) % values.shape[longest]
        spots.append(tuple(where))
    return values.at[spots[0]].set(smallest).at[spots[1]].set(high)


def levels(key, dims, shards, low, top_value):
    factor_of = 1.0
    for axis_at, parts in shards:
        steps = jax.random.uniform(jax.random.fold_in(jax.random.fold_in(key, 6), axis_at), (parts,), jnp.float32, low / len(shards), top_value / len(shards))
        factor_of = factor_of * jnp.repeat(jnp.exp(steps), dims[axis_at] // parts).reshape((-1,) + (1,) * (len(dims) - 1 - axis_at))
    return factor_of


def scatter_about(key, extent, spread, bound, cuts=(), kind=jnp.bfloat16):
    level = levels(key, extent, cuts, -0.22, 0.18) if cuts else 1.0
    drawn = jax.random.normal(key, extent, jnp.float32) * spread * level
    return jnp.minimum(jnp.maximum(drawn, -bound), bound).astype(kind)


def setup_inputs(seed: int = 0) -> dict:
    seeds = jax.random.split(jax.random.key(seed), 6)
    right_side = scatter_about(seeds[0], (NZ, 3, NY, NX), 1.0, 6.0, ((0, 2), (2, 4), (3, 4)), jnp.float32)
    start_field = scatter_about(seeds[1], (NZ, 3, NY, NX), 1.0, 6.0, ((0, 2), (2, 4), (3, 4)), jnp.float32)
    layer_material = touch_ends(jax.random.randint(seeds[2], (NZ,), 0, MATS), jax.random.fold_in(seeds[2], 1), 0, MATS - 1).astype(jnp.int32)
    stiffness = draw_stiffness(jax.random.fold_in(seeds[5], 71), 0)
    line_factors = draw_line_factors(jax.random.fold_in(seeds[5], 71), 0)
    return dict(right_side=right_side, start_field=start_field, layer_material=layer_material, stiffness=stiffness, line_factors=line_factors)


def apply_block(blocks, field):
    columns = []
    for row_index in range(3):
        summed = blocks[..., row_index, 0, None, None] * field[..., 0, :, :]
        for col_index in (1, 2):
            summed = summed + blocks[..., row_index, col_index, None, None] * field[..., col_index, :, :]
        columns.append(summed)
    return jnp.stack(columns, axis=-3)


def operate(field, diag_block, lateral_block, vertical_block):
    padded = jnp.pad(field, ((1, 1), (0, 0), (1, 1), (1, 1)))
    lateral = padded[1:-1, :, 1:-1, 2:] + padded[1:-1, :, 1:-1, :-2]
    lateral = lateral + padded[1:-1, :, 2:, 1:-1] + padded[1:-1, :, :-2, 1:-1]
    vertical = padded[2:, :, 1:-1, 1:-1] + padded[:-2, :, 1:-1, 1:-1]
    return apply_block(diag_block, field) - apply_block(lateral_block, lateral) - apply_block(vertical_block, vertical)


def line_solve(resid, factor_blocks):
    weighted = apply_block(factor_blocks[:, 0], resid)

    def advance(carry, item):
        multiplier, source = item
        nxt = source + apply_block(multiplier, carry)
        return nxt, nxt

    start = jnp.zeros(resid.shape[1:], jnp.float32)
    _, upward = lax.scan(advance, start, (factor_blocks[:, 1], weighted))
    _, downward = lax.scan(advance, start, (factor_blocks[:, 2], upward), reverse=True)
    return downward


def reference(right_side, start_field, layer_material, stiffness, line_factors):
    fine_sten = stiffness[layer_material]
    coarse_ids = layer_material[0::2]
    coarse_sten = stiffness[coarse_ids]
    fine_fac = line_factors[layer_material]
    coarse_fac = line_factors[coarse_ids]
    fine_args = (fine_sten[:, 0], fine_sten[:, 1], fine_sten[:, 2])
    coarse_args = (coarse_sten[:, 0], coarse_sten[:, 1], 0.25 * coarse_sten[:, 2])
    field = start_field
    for counter in range(SWEEPS):
        field = field + line_solve(right_side - operate(field, *fine_args), fine_fac)
    resid = right_side - operate(field, *fine_args)
    paired = resid.reshape(resid.shape[0] // 2, 2, 3, resid.shape[2], resid.shape[3])
    coarse_rhs = paired[:, 0] + paired[:, 1]
    correction = line_solve(coarse_rhs, coarse_fac)
    for counter in range(SWEEPS - 1):
        correction = correction + line_solve(coarse_rhs - operate(correction, *coarse_args), coarse_fac)
    solution_field = field + jnp.repeat(correction, 2, axis=0)
    final_residual = right_side - operate(solution_field, *fine_args)
    return solution_field, final_residual
```

```python
import functools

import jax
import jax.numpy as jnp
from jax import lax
from jax.experimental import pallas as pl
from jax.experimental.pallas import tpu as pltpu
from jax.sharding import PartitionSpec as P

SWEEPS = 3
REACH = 2 * SWEEPS + 1
POWERS = REACH + 1
SLOT = 8
MESH = pl.DeviceIdType.MESH


def total(terms):
    result = terms[0]
    for term in terms[1:]:
        result = result + term
    return result


def kernel(
    sizes, dims, material, sten, fac, load, start, out_u, out_r,
    mats, own_u, own_b, prev_u, prev_b, next_u, next_b, edge_out, edge_in, work, keep,
    sym_u, sym_b, sym_r, sym_y, sym_e, sym_c, maps, left, right, mine, outgoing, incoming,
    mat_ss, mat_rs, row_ss, row_rs, edge_ss, edge_rs, part_ss, part_rs,
):
    nz, ny, nx = sizes
    layers, comps, rows, lanes = dims
    planes = layers * comps
    deep = nz * layers
    width = lanes + 128
    gz, gy, gx = (lax.axis_index(name) for name in ("gz", "gy", "gx"))
    three = range(comps)
    group = right.shape[1] // POWERS
    half_group = group // 2
    pending = []

    def at(z, y, x):
        return {"gz": z, "gy": y, "gx": x}

    def copy_if(cond, src, dst, ss, rs, target):
        copy = pltpu.make_async_remote_copy(
            src_ref=src, dst_ref=dst, send_sem=ss, recv_sem=rs,
            device_id=target, device_id_type=MESH,
        )

        @pl.when(cond)
        def _():
            copy.start()

        pending.append((cond, copy))

    def arrive_if(cond, ref, ss, rs):
        @pl.when(cond)
        def _():
            pltpu.make_async_remote_copy(
                src_ref=ref, dst_ref=ref, send_sem=ss, recv_sem=rs,
                device_id=at(gz, gy, gx), device_id_type=MESH,
            ).wait_recv()

    has_prev_y, has_next_y = gy > 0, gy < ny - 1
    has_prev_x, has_next_x = gx > 0, gx < nx - 1
    sides_y = ((-1, has_prev_y), (0, True), (1, has_next_y))
    sides_x = ((-1, has_prev_x), (1, has_next_x))

    barrier = pltpu.get_barrier_semaphore()
    peers = [(gz != j, at(j, gy, gx)) for j in range(nz)]
    peers += [(cond, at(gz, gy + step, gx)) for step, cond in sides_y if step]
    for step_y, cond_y in sides_y:
        for step_x, cond_x in sides_x:
            peers.append((jnp.logical_and(cond_y, cond_x), at(gz, gy + step_y, gx + step_x)))
    for cond, target in peers:
        @pl.when(cond)
        def _(target=target):
            pl.semaphore_signal(barrier, inc=1, device_id=target, device_id_type=MESH)

    tiles = lanes // 128
    for own, given in ((own_u, start), (own_b, load)):
        for y in range(rows):
            for tile in range(tiles):
                own[y, :, tile * 128 : (tile + 1) * 128] = given[pl.ds(tile * rows + y, planes, stride=tiles * rows), :]

    def place(index):
        return (index * SLOT // 128) * 128, index * SLOT % 128

    tile_lane = lax.broadcasted_iota(jnp.int32, (planes, 128), 1)
    for side in range(2):
        for tile in range(edge_out.shape[2] // 128):
            packed = jnp.zeros((planes, 128), jnp.float32)
            for which, ref in enumerate((own_u, own_b)):
                for y in range(rows):
                    base, spot = place(which * rows + y)
                    if base != tile * 128:
                        continue
                    if side == 0:
                        piece = pltpu.roll(ref[y, :, 0:128], spot, 1) if spot else ref[y, :, 0:128]
                    else:
                        piece = pltpu.roll(ref[y, :, lanes - 128 : lanes], (spot + SLOT) % 128, 1)
                    inside = jnp.logical_and(tile_lane >= spot, tile_lane < spot + SLOT)
                    packed = jnp.where(inside, piece, packed)
            edge_out[side, :, tile * 128 : (tile + 1) * 128] = packed

    pl.semaphore_wait(barrier, total([cond.astype(jnp.int32) for cond, _ in peers]))

    for j in range(nz):
        copy_if(gz != j, material, mats.at[gz], mat_ss.at[j], mat_rs.at[gz], at(j, gy, gx))
    for step_y, cond_y in sides_y:
        for side, (step_x, cond_x) in enumerate(sides_x):
            slot = edge_in.at[1 - side, 1 - step_y]
            copy_if(jnp.logical_and(cond_y, cond_x), edge_out.at[side], slot,
                    edge_ss.at[1 - side, 1 - step_y], edge_rs.at[1 - side, 1 - step_y],
                    at(gz, gy + step_y, gx + step_x))
    strips = ((own_u, prev_u, next_u, REACH), (own_b, prev_b, next_b, REACH - 1))
    for which, (own, prev, after, depth) in enumerate(strips):
        copy_if(has_next_y, own.at[rows - depth : rows], prev,
                row_ss.at[which, 0], row_rs.at[which, 0], at(gz, gy + 1, gx))
        copy_if(has_prev_y, own.at[0:depth], after,
                row_ss.at[which, 1], row_rs.at[which, 1], at(gz, gy - 1, gx))

    for layer in range(layers):
        mats[gz, layer] = material[layer]
    for cond, refs in ((has_prev_y, (prev_u, prev_b)), (has_next_y, (next_u, next_b))):
        @pl.when(jnp.logical_not(cond))
        def _(refs=refs):
            for ref in refs:
                ref[...] = jnp.zeros_like(ref)
    for step_y, cond_y in sides_y:
        for side, (step_x, cond_x) in enumerate(sides_x):
            @pl.when(jnp.logical_not(jnp.logical_and(cond_y, cond_x)))
            def _(side=side, step_y=step_y):
                edge_in[side, 1 + step_y] = jnp.zeros_like(edge_in[side, 1 + step_y])
    wide_lane = lax.broadcasted_iota(jnp.int32, (planes, width), 1)
    inner = (wide_lane < lanes).astype(jnp.float32)
    inner = inner + jnp.where(
        jnp.logical_and(wide_lane >= lanes, wide_lane < lanes + SLOT), has_next_x.astype(jnp.float32), 0.0)
    inner = inner + jnp.where(wide_lane >= width - SLOT, has_prev_x.astype(jnp.float32), 0.0)
    keep[0] = inner * has_prev_y.astype(jnp.float32)
    keep[1] = inner
    keep[2] = inner * has_next_y.astype(jnp.float32)
    for y in range(rows):
        for power in range(POWERS):
            for part in range(2):
                if power == REACH and part == 1:
                    low = 0
                else:
                    low = planes
                if low < half_group:
                    first = power * group + part * half_group + low
                    stop = power * group + (part + 1) * half_group
                    right[y, first:stop, :] = jnp.zeros((stop - first, lanes), jnp.float32)

    sub = lax.broadcasted_iota(jnp.int32, (8, 128), 0)
    lane = lax.broadcasted_iota(jnp.int32, (8, 128), 1)
    lowest = sub == 0

    def block(table, level, layer, which):
        z = layer * (2 if level else 1)
        mat_id = mats[z // layers, z % layers]
        values = [[table[which, i, j, mat_id] for j in three] for i in three]
        if level and table is sten and which == 2:
            values = [[0.25 * v for v in line] for line in values]
        return values

    def times(mat, vec):
        return [total([mat[i][j] * vec[j] for j in three]) for i in three]

    def spread(x):
        return jnp.where(lowest, 0.0, pltpu.roll(x, 1, 0))

    for z in range(deep):
        here = gz == z // layers
        for c in three:
            plane = z % layers * comps + c
            spot = jnp.where(here, plane, -1 - half_group)
            sym_u[z * comps + c] = jnp.logical_and(lowest, lane == spot).astype(jnp.float32)
            sym_b[z * comps + c] = jnp.logical_and(lowest, lane == spot + half_group).astype(jnp.float32)

    def residual(level, field, source, count, layer):
        here = [field[layer * comps + c] for c in three]
        side = [spread(x) for x in here]
        vert = []
        for c in three:
            near = []
            if layer:
                near.append(field[(layer - 1) * comps + c])
            if layer < count - 1:
                near.append(field[(layer + 1) * comps + c])
            vert.append(total(near))
        a = times(block(sten, level, layer, 0), here)
        b = times(block(sten, level, layer, 1), side)
        d = times(block(sten, level, layer, 2), vert)
        return [source[layer * comps + c] - (a[c] - b[c] - d[c]) for c in three]

    def line_solve(level, resid, field, count, fresh):
        carry = None
        for layer in range(count):
            now = times(block(fac, level, layer, 0), resid(layer))
            if carry is not None:
                now = [a + b for a, b in zip(now, times(block(fac, level, layer, 1), carry))]
            for c in three:
                sym_y[layer * comps + c] = now[c]
            carry = now
        back = None
        for layer in reversed(range(count)):
            now = [sym_y[layer * comps + c] for c in three]
            if back is not None:
                now = [a + b for a, b in zip(now, times(block(fac, level, layer, 2), back))]
            for c in three:
                spot = layer * comps + c
                field[spot] = now[c] if fresh else field[spot] + now[c]
            back = now

    for j in range(nz):
        arrive_if(gz != j, mats.at[j], mat_ss.at[j], mat_rs.at[j])
    for sweep in range(SWEEPS):
        line_solve(0, lambda layer: residual(0, sym_u, sym_b, deep, layer), sym_u, deep, False)
    for k in range(deep // 2):
        pair = [residual(0, sym_u, sym_b, deep, 2 * k + step) for step in range(2)]
        for c in three:
            sym_c[k * comps + c] = pair[0][c] + pair[1][c]
    for sweep in range(SWEEPS):
        if sweep:
            source = functools.partial(residual, 1, sym_e, sym_c, deep // 2)
        else:
            def source(layer):
                return [sym_c[layer * comps + c] for c in three]
        line_solve(1, source, sym_e, deep // 2, sweep == 0)
    for z in range(deep):
        for c in three:
            sym_u[z * comps + c] = sym_u[z * comps + c] + sym_e[z // 2 * comps + c]
    for z in range(deep):
        value = residual(0, sym_u, sym_b, deep, z)
        first = z // layers * 2 * planes + z % layers * comps
        for c in three:
            maps[(first + c) * 8 : (first + c + 1) * 8, :] = sym_u[z * comps + c]
            spot = first + planes + c
            maps[spot * 8 : (spot + 1) * 8, :] = value[c]
    for i in range(nz):
        target = lax.rem(gz + 1 + i, nz)
        for pair in range(POWERS * group // 128):
            tile = None
            for part in range(128 // group):
                power = pair * (128 // group) + part
                value = maps[pl.ds(target * 2 * planes * 8 + power, 2 * planes, stride=8), :]
                if part:
                    value = pltpu.roll(value, part * group, 1)
                tile = value if tile is None else tile + value
            left[i * 2 * planes : (i + 1) * 2 * planes, pair * 128 : (pair + 1) * 128] = tile

    for step_y, cond_y in sides_y:
        for side, (step_x, cond_x) in enumerate(sides_x):
            arrive_if(jnp.logical_and(cond_y, cond_x), edge_in.at[side, 1 + step_y],
                      edge_ss.at[side, 1 + step_y], edge_rs.at[side, 1 + step_y])

    def powers(which):
        own, prev, after, depth = strips[which]
        arrive_if(has_prev_y, prev, row_ss.at[which, 0], row_rs.at[which, 0])
        arrive_if(has_next_y, after, row_ss.at[which, 1], row_rs.at[which, 1])

        def raw(y):
            if y < 0:
                middle, step_y, line = prev[depth + y], -1, rows + y
            elif y < rows:
                middle, step_y, line = own[y], 0, y
            else:
                middle, step_y, line = after[y - rows], 1, y - rows
            base, spot = place(which * rows + line)
            west = pltpu.roll(edge_in[0, 1 + step_y, :, base : base + 128], (128 - SLOT - spot) % 128, 1)
            east = edge_in[1, 1 + step_y, :, base : base + 128]
            if spot:
                east = pltpu.roll(east, 128 - spot, 1)
            tail = jnp.where(tile_lane < SLOT, east, jnp.where(tile_lane >= 128 - SLOT, west, 0.0))
            return jnp.concatenate([middle, tail], axis=1)

        for power in range(depth + 1):
            reach = depth - power
            now = work.at[power % 2]
            old = work.at[1 - power % 2]
            for y in range(-reach, rows + reach):
                if power == 0:
                    value = raw(y)
                else:
                    x = old[y + REACH]
                    value = pltpu.roll(x, 1, 1) + pltpu.roll(x, width - 1, 1)
                    value = value + (old[y + REACH - 1] + old[y + REACH + 1])
                    value = value * keep[0 if y < 0 else 1 if y < rows else 2]
                now[y + REACH] = value
                if 0 <= y < rows:
                    first = power * group + which * half_group
                    right[y, first : first + planes, :] = value[:, :lanes]

    powers(0)
    powers(1)

    size = 2 * planes
    for y in range(rows):
        value = jnp.dot(left[...], right[y], precision=lax.Precision.HIGHEST, preferred_element_type=jnp.float32)
        for i in range(nz - 1):
            outgoing[i, y] = value[i * size : (i + 1) * size]
            copy_if(True, outgoing.at[i, y], incoming.at[i, y],
                    part_ss.at[i, y], part_rs.at[i, y], at(lax.rem(gz + 1 + i, nz), gy, gx))
        mine[y] = value[(nz - 1) * size :]
    for y in range(rows):
        value = mine[y]
        for i in range(nz - 1):
            arrive_if(True, incoming.at[i, y], part_ss.at[i, y], part_rs.at[i, y])
            value = value + incoming[i, y]
        for tile in range(tiles):
            part = value[:, tile * 128 : (tile + 1) * 128]
            spots = pl.ds(tile * rows + y, planes, stride=tiles * rows)
            out_u[spots, :] = part[:planes]
            out_r[spots, :] = part[planes:]
    for cond, copy in pending:
        @pl.when(cond)
        def _(copy=copy):
            copy.wait_send()


def solution(mesh):
    sizes = tuple(mesh.shape[name] for name in ("gz", "gy", "gx"))
    nz = sizes[0]

    def on_device(right_side, start_field, layer_material, stiffness, line_factors):
        dims = right_side.shape
        layers, comps, rows, lanes = dims
        planes = layers * comps
        deep = nz * layers
        half_group = -(-planes // 32) * 32
        depth = POWERS * 2 * half_group
        packed = -(-2 * rows * SLOT // 128) * 128
        f32 = jnp.float32
        vmem = pl.BlockSpec(memory_space=pltpu.VMEM)
        smem = pl.BlockSpec(memory_space=pltpu.SMEM)
        dma = pltpu.SemaphoreType.DMA
        others = max(nz - 1, 1)
        symbol = pltpu.VMEM((deep * comps, 8, 128), f32)
        scratch = [pltpu.SMEM((nz, layers), jnp.int32)]
        scratch += [pltpu.VMEM((rows, planes, lanes), f32)] * 2
        scratch += [pltpu.VMEM((n, planes, lanes), f32) for n in (REACH, REACH - 1, REACH, REACH - 1)]
        scratch += [
            pltpu.VMEM((2, planes, packed), f32),
            pltpu.VMEM((2, 3, planes, packed), f32),
            pltpu.VMEM((2, rows + 2 * REACH, planes, lanes + 128), f32),
            pltpu.VMEM((3, planes, lanes + 128), f32),
        ]
        scratch += [symbol] * 6
        scratch += [
            pltpu.VMEM((nz * 2 * planes * 8, 128), f32),
            pltpu.VMEM((nz * 2 * planes, depth), f32),
            pltpu.VMEM((rows, depth, lanes), f32),
            pltpu.VMEM((rows, 2 * planes, lanes), f32),
            pltpu.VMEM((others, rows, 2 * planes, lanes), f32),
            pltpu.VMEM((others, rows, 2 * planes, lanes), f32),
        ]
        scratch += [dma((nz,))] * 2 + [dma((2, 2))] * 2 + [dma((2, 3))] * 2 + [dma((others, rows))] * 2
        tiled = (layers, comps, rows, lanes // 128, 128)

        def flatten(x):
            return x.reshape(tiled).transpose(0, 1, 3, 2, 4).reshape(-1, 128)

        def unflatten(x):
            split = x.reshape(layers, comps, lanes // 128, rows, 128)
            return split.transpose(0, 1, 3, 2, 4).reshape(dims)

        out = jax.ShapeDtypeStruct((planes * rows * lanes // 128, 128), f32)
        outs = pl.pallas_call(
            functools.partial(kernel, sizes, dims),
            out_shape=(out, out),
            in_specs=[smem, smem, smem, vmem, vmem],
            out_specs=(vmem, vmem),
            scratch_shapes=scratch,
            compiler_params=pltpu.CompilerParams(
                collective_id=0, has_side_effects=True, vmem_limit_bytes=VMEM_LIMIT),
        )(layer_material, stiffness.transpose(1, 2, 3, 0), line_factors.transpose(1, 2, 3, 0),
          flatten(right_side), flatten(start_field))
        return tuple(unflatten(o) for o in outs)

    return jax.shard_map(
        on_device,
        mesh=mesh,
        in_specs=(P("gz", None, "gy", "gx"), P("gz", None, "gy", "gx"), P("gz"), P(), P()),
        out_specs=(P("gz", None, "gy", "gx"), P("gz", None, "gy", "gx")),
        check_vma=False,
    )


VMEM_LIMIT = 40 * 1024 * 1024
```

```python
import functools

import jax
import jax.numpy as jnp
from jax import lax
from jax.experimental import pallas as pl
from jax.experimental.pallas import tpu as pltpu
from jax.sharding import PartitionSpec as P

SWEEPS = 3
REACH = 2 * SWEEPS + 1
POWERS = REACH + 1
SLOT = 8
MESH = pl.DeviceIdType.MESH


def total(terms):
    result = terms[0]
    for term in terms[1:]:
        result = result + term
    return result


def kernel(
    sizes, dims, material_hbm, sten_hbm, fac_hbm, load_hbm, start_hbm, out_u, out_r,
    material, sten, fac, load, start, coef, in_sem,
    mats, own_u, own_b, prev_u, prev_b, next_u, next_b, edge_out, edge_in, work_u, work_b, keep,
    sym_u, sym_b, sym_r, sym_y, sym_e, sym_c, maps, left, right, mine, outgoing, incoming,
    mat_ss, mat_rs, row_ss, row_rs, edge_ss, edge_rs, part_ss, part_rs,
):
    nz, ny, nx = sizes
    layers, comps, rows, lanes = dims
    planes = layers * comps
    deep = nz * layers
    width = lanes + 128
    gz, gy, gx = (lax.axis_index(name) for name in ("gz", "gy", "gx"))
    three = range(comps)
    half_group = -(-planes // 32) * 32
    depth = POWERS * half_group
    pending = []
    fetches = [
        pltpu.make_async_copy(src, dst, in_sem.at[i])
        for i, (src, dst) in enumerate((
            (start_hbm, start), (load_hbm, load), (sten_hbm, sten), (fac_hbm, fac), (material_hbm, material),
        ))
    ]
    for fetch in fetches:
        fetch.start()

    def at(z, y, x):
        return {"gz": z, "gy": y, "gx": x}

    def copy_if(cond, src, dst, ss, rs, target):
        copy = pltpu.make_async_remote_copy(
            src_ref=src, dst_ref=dst, send_sem=ss, recv_sem=rs,
            device_id=target, device_id_type=MESH,
        )

        if cond is True:
            copy.start()
        else:
            @pl.when(cond)
            def _():
                copy.start()

        pending.append((cond, copy))

    def arrive_if(cond, ref, ss, rs):
        copy = pltpu.make_async_remote_copy(
            src_ref=ref, dst_ref=ref, send_sem=ss, recv_sem=rs,
            device_id=at(gz, gy, gx), device_id_type=MESH,
        )
        if cond is True:
            copy.wait_recv()
        else:
            @pl.when(cond)
            def _():
                copy.wait_recv()

    has_prev_y, has_next_y = gy > 0, gy < ny - 1
    has_prev_x, has_next_x = gx > 0, gx < nx - 1
    sides_y = ((-1, has_prev_y), (0, True), (1, has_next_y))
    sides_x = ((-1, has_prev_x), (1, has_next_x))

    barrier = pltpu.get_barrier_semaphore()
    peers = [(gz != j, at(j, gy, gx)) for j in range(nz)]
    peers += [(cond, at(gz, gy + step, gx)) for step, cond in sides_y if step]
    for step_y, cond_y in sides_y:
        for step_x, cond_x in sides_x:
            peers.append((jnp.logical_and(cond_y, cond_x), at(gz, gy + step_y, gx + step_x)))
    for cond, target in peers:
        @pl.when(cond)
        def _(target=target):
            pl.semaphore_signal(barrier, inc=1, device_id=target, device_id_type=MESH)

    tiles = lanes // 128
    for own, given, fetch in ((own_u, start, fetches[0]), (own_b, load, fetches[1])):
        fetch.wait()
        for y in range(rows):
            for tile in range(tiles):
                own[y, :, tile * 128 : (tile + 1) * 128] = given[pl.ds(tile * rows + y, planes, stride=tiles * rows), :]

    def place(index):
        return (index * SLOT // 128) * 128, index * SLOT % 128

    tile_lane = lax.broadcasted_iota(jnp.int32, (planes, 128), 1)
    for side in range(2):
        for tile in range(edge_out.shape[2] // 128):
            packed = jnp.zeros((planes, 128), jnp.float32)
            for which, ref in enumerate((own_u, own_b)):
                for y in range(rows):
                    base, spot = place(which * rows + y)
                    if base != tile * 128:
                        continue
                    if side == 0:
                        piece = pltpu.roll(ref[y, :, 0:128], spot, 1) if spot else ref[y, :, 0:128]
                    else:
                        piece = pltpu.roll(ref[y, :, lanes - 128 : lanes], (spot + SLOT) % 128, 1)
                    inside = jnp.logical_and(tile_lane >= spot, tile_lane < spot + SLOT)
                    packed = jnp.where(inside, piece, packed)
            edge_out[side, :, tile * 128 : (tile + 1) * 128] = packed

    fetches[4].wait()
    pl.semaphore_wait(barrier, total([cond.astype(jnp.int32) for cond, _ in peers]))

    for j in range(nz):
        copy_if(gz != j, material, mats.at[gz], mat_ss.at[j], mat_rs.at[gz], at(j, gy, gx))
    for step_y, cond_y in sides_y:
        for side, (step_x, cond_x) in enumerate(sides_x):
            slot = edge_in.at[1 - side, 1 - step_y]
            copy_if(jnp.logical_and(cond_y, cond_x), edge_out.at[side], slot,
                    edge_ss.at[1 - side, 1 - step_y], edge_rs.at[1 - side, 1 - step_y],
                    at(gz, gy + step_y, gx + step_x))
    strips = ((own_u, prev_u, next_u, REACH), (own_b, prev_b, next_b, REACH - 1))
    stages = rows // 2

    def known(which, stage):
        return max(strips[which][3] - stages + 1 + stage, 0)

    def strip(which, stage):
        own, prev, after, reach = strips[which]
        first = known(which, stage - 1) if stage else 0
        last = known(which, stage)
        return ((own.at[rows - last : rows - first], prev.at[reach - last : reach - first]),
                (own.at[first:last], after.at[first:last]))

    for stage in range(stages):
        for which in range(2):
            (out_up, in_up), (out_down, in_down) = strip(which, stage)
            copy_if(has_next_y, out_up, in_up,
                    row_ss.at[which, stage, 0], row_rs.at[which, stage, 0], at(gz, gy + 1, gx))
            copy_if(has_prev_y, out_down, in_down,
                    row_ss.at[which, stage, 1], row_rs.at[which, stage, 1], at(gz, gy - 1, gx))

    for layer in range(layers):
        mats[gz, layer] = material[layer]
    blocks = 3 * comps * comps
    for fetch in fetches[2:4]:
        fetch.wait()
    for first, table in ((0, sten), (blocks, fac)):
        for which in range(3):
            for i in three:
                for j in three:
                    for mat_id in range(coef.shape[0]):
                        spot = first + (which * comps + i) * comps + j
                        coef[mat_id, spot] = jnp.full((8, 128), table[which, i, j, mat_id], jnp.float32)
    for cond, refs in ((has_prev_y, (prev_u, prev_b)), (has_next_y, (next_u, next_b))):
        @pl.when(jnp.logical_not(cond))
        def _(refs=refs):
            for ref in refs:
                ref[...] = jnp.zeros_like(ref)
    for step_y, cond_y in sides_y:
        for side, (step_x, cond_x) in enumerate(sides_x):
            @pl.when(jnp.logical_not(jnp.logical_and(cond_y, cond_x)))
            def _(side=side, step_y=step_y):
                edge_in[side, 1 + step_y] = jnp.zeros_like(edge_in[side, 1 + step_y])
    wide_lane = lax.broadcasted_iota(jnp.int32, (planes, width), 1)
    inner = (wide_lane < lanes).astype(jnp.float32)
    inner = inner + jnp.where(
        jnp.logical_and(wide_lane >= lanes, wide_lane < lanes + SLOT), has_next_x.astype(jnp.float32), 0.0)
    inner = inner + jnp.where(wide_lane >= width - SLOT, has_prev_x.astype(jnp.float32), 0.0)
    keep[0] = inner * has_prev_y.astype(jnp.float32)
    keep[1] = inner
    keep[2] = inner * has_next_y.astype(jnp.float32)
    for part in range(3):
        for y in range(rows):
            right[part, y, 2 * depth - half_group :, :] = jnp.zeros((half_group, lanes), jnp.bfloat16)

    sub = lax.broadcasted_iota(jnp.int32, (8, 128), 0)
    lane = lax.broadcasted_iota(jnp.int32, (8, 128), 1)
    lowest = sub == 0

    def block(table, level, layer, which):
        z = layer * (2 if level else 1)
        mat_id = mats[z // layers, z % layers]
        first = which * comps * comps + (blocks if table is fac else 0)
        return [[coef[mat_id, first + i * comps + j] for j in three] for i in three]

    def times(mat, vec):
        return [total([mat[i][j] * vec[j] for j in three]) for i in three]

    def spread(x):
        return jnp.where(lowest, 0.0, pltpu.roll(x, 1, 0))

    for z in range(deep):
        here = gz == z // layers
        for c in three:
            plane = z % layers * comps + c
            spot = jnp.where(here, plane, -1 - half_group)
            sym_u[z * comps + c] = jnp.logical_and(lowest, lane == spot).astype(jnp.float32)
            sym_b[z * comps + c] = jnp.logical_and(lowest, lane == spot + half_group).astype(jnp.float32)

    def residual(level, field, source, count, layer):
        here = [field[layer * comps + c] for c in three]
        side = [spread(x) for x in here]
        vert = []
        for c in three:
            near = []
            if layer:
                near.append(field[(layer - 1) * comps + c])
            if layer < count - 1:
                near.append(field[(layer + 1) * comps + c])
            vert.append(0.25 * total(near) if level else total(near))
        a = times(block(sten, level, layer, 0), here)
        b = times(block(sten, level, layer, 1), side)
        d = times(block(sten, level, layer, 2), vert)
        return [source[layer * comps + c] - (a[c] - b[c] - d[c]) for c in three]

    def line_solve(level, resid, field, count, fresh):
        carry = None
        for layer in range(count):
            now = times(block(fac, level, layer, 0), resid(layer))
            if carry is not None:
                now = [a + b for a, b in zip(now, times(block(fac, level, layer, 1), carry))]
            for c in three:
                sym_y[layer * comps + c] = now[c]
            carry = now
        back = None
        for layer in reversed(range(count)):
            now = [sym_y[layer * comps + c] for c in three]
            if back is not None:
                now = [a + b for a, b in zip(now, times(block(fac, level, layer, 2), back))]
            for c in three:
                spot = layer * comps + c
                field[spot] = now[c] if fresh else field[spot] + now[c]
            back = now

    for j in range(nz):
        arrive_if(gz != j, mats.at[j], mat_ss.at[j], mat_rs.at[j])
    for sweep in range(SWEEPS):
        line_solve(0, lambda layer: residual(0, sym_u, sym_b, deep, layer), sym_u, deep, False)
    for k in range(deep // 2):
        pair = [residual(0, sym_u, sym_b, deep, 2 * k + step) for step in range(2)]
        for c in three:
            sym_c[k * comps + c] = pair[0][c] + pair[1][c]
    for sweep in range(SWEEPS):
        if sweep:
            source = functools.partial(residual, 1, sym_e, sym_c, deep // 2)
        else:
            def source(layer):
                return [sym_c[layer * comps + c] for c in three]
        line_solve(1, source, sym_e, deep // 2, sweep == 0)
    for z in range(deep):
        for c in three:
            sym_u[z * comps + c] = sym_u[z * comps + c] + sym_e[z // 2 * comps + c]
    for z in range(deep):
        value = residual(0, sym_u, sym_b, deep, z)
        first = z // layers * 2 * planes + z % layers * comps
        for c in three:
            maps[(first + c) * 8 : (first + c + 1) * 8, :] = sym_u[z * comps + c]
            spot = first + planes + c
            maps[spot * 8 : (spot + 1) * 8, :] = value[c]
    def thirds(x):
        high = x.astype(jnp.bfloat16)
        rest = x - high.astype(jnp.float32)
        middle = rest.astype(jnp.bfloat16)
        return high, middle, (rest - middle.astype(jnp.float32)).astype(jnp.bfloat16)

    size = 2 * planes
    count = nz * size
    map_lane = lax.broadcasted_iota(jnp.int32, (size, 128), 1)
    for i in range(nz):
        target = lax.rem(gz + 1 + i, nz)
        lines = [maps[pl.ds(target * size * 8 + power, size, stride=8), :] for power in range(POWERS)]
        for which in range(2):
            base = which * half_group
            inside = jnp.logical_and(map_lane >= base, map_lane < base + half_group)
            each = 128 // half_group
            for tile in range(POWERS // each):
                value = jnp.zeros((size, 128), jnp.float32)
                for part in range(each):
                    piece = jnp.where(inside, lines[tile * each + part], 0.0)
                    shift = (part * half_group - base) % 128
                    value = value + (pltpu.roll(piece, shift, 1) if shift else piece)
                first = which * depth + tile * 128
                for part, third in enumerate(thirds(value)):
                    left[part * count + i * size : part * count + (i + 1) * size, first : first + 128] = third

    for step_y, cond_y in sides_y:
        for side, (step_x, cond_x) in enumerate(sides_x):
            arrive_if(jnp.logical_and(cond_y, cond_x), edge_in.at[side, 1 + step_y],
                      edge_ss.at[side, 1 + step_y], edge_rs.at[side, 1 + step_y])

    def raw(which, y):
        own, prev, after, reach = strips[which]
        if y < 0:
            middle, step_y, line = prev[reach + y], -1, rows + y
        elif y < rows:
            middle, step_y, line = own[y], 0, y
        else:
            middle, step_y, line = after[y - rows], 1, y - rows
        base, spot = place(which * rows + line)
        west = pltpu.roll(edge_in[0, 1 + step_y, :, base : base + 128], (128 - SLOT - spot) % 128, 1)
        east = edge_in[1, 1 + step_y, :, base : base + 128]
        if spot:
            east = pltpu.roll(east, 128 - spot, 1)
        tail = jnp.where(tile_lane < SLOT, east, jnp.where(tile_lane >= 128 - SLOT, west, 0.0))
        return jnp.concatenate([middle, tail], axis=1)

    padding = jnp.zeros((half_group - planes, lanes), jnp.float32)
    done = set()

    def extend(which, known_rows):
        work, reach = (work_u, work_b)[which], strips[which][3]
        for power in range(reach + 1):
            for y in range(power - known_rows, rows + known_rows - power):
                if (which, power, y) in done:
                    continue
                done.add((which, power, y))
                if power == 0:
                    value = raw(which, y)
                else:
                    x = work[power - 1, y + reach]
                    value = pltpu.roll(x, 1, 1) + pltpu.roll(x, width - 1, 1)
                    value = value + (work[power - 1, y + reach - 1] + work[power - 1, y + reach + 1])
                    value = value * keep[0 if y < 0 else 1 if y < rows else 2]
                if power < reach:
                    work[power, y + reach] = value
                if 0 <= y < rows:
                    first = which * depth + power * half_group
                    cell = value[:, :lanes]
                    if half_group > planes:
                        cell = jnp.concatenate([cell, padding], axis=0)
                    for part, third in enumerate(thirds(cell)):
                        right[part, y, first : first + half_group, :] = third

    for which in range(2):
        extend(which, 0)
    for stage in range(stages):
        for which in range(2):
            (_, in_up), (_, in_down) = strip(which, stage)
            arrive_if(has_prev_y, in_up, row_ss.at[which, stage, 0], row_rs.at[which, stage, 0])
            arrive_if(has_next_y, in_down, row_ss.at[which, stage, 1], row_rs.at[which, stage, 1])
        for which in range(2):
            extend(which, known(which, stage))
        for y in (stages - 1 - stage, stages + stage):
            pieces = []
            for part in (2, 1, 0):
                product = jnp.dot(left[: (3 - part) * count], right[part, y], preferred_element_type=jnp.float32)
                pieces += [product[k * count : (k + 1) * count] for k in reversed(range(3 - part))]
            value = total(pieces)
            for i in range(nz - 1):
                outgoing[i, y] = value[i * size : (i + 1) * size]
                copy_if(True, outgoing.at[i, y], incoming.at[i, y],
                        part_ss.at[i, y], part_rs.at[i, y], at(lax.rem(gz + 1 + i, nz), gy, gx))
            mine[y] = value[(nz - 1) * size :]
    for y in [y for stage in range(stages) for y in (stages - 1 - stage, stages + stage)]:
        value = mine[y]
        for i in range(nz - 1):
            arrive_if(True, incoming.at[i, y], part_ss.at[i, y], part_rs.at[i, y])
            value = value + incoming[i, y]
        for tile in range(tiles):
            part = value[:, tile * 128 : (tile + 1) * 128]
            spots = pl.ds(tile * rows + y, planes, stride=tiles * rows)
            out_u[spots, :] = part[:planes]
            out_r[spots, :] = part[planes:]
    for cond, copy in pending:
        if cond is True:
            copy.wait_send()
        else:
            @pl.when(cond)
            def _(copy=copy):
                copy.wait_send()


def solution(mesh):
    sizes = tuple(mesh.shape[name] for name in ("gz", "gy", "gx"))
    nz = sizes[0]

    def on_device(right_side, start_field, layer_material, stiffness, line_factors):
        dims = right_side.shape
        layers, comps, rows, lanes = dims
        planes = layers * comps
        deep = nz * layers
        half_group = -(-planes // 32) * 32
        depth = POWERS * 2 * half_group
        packed = -(-2 * rows * SLOT // 128) * 128
        f32 = jnp.float32
        vmem = pl.BlockSpec(memory_space=pltpu.VMEM)
        dma = pltpu.SemaphoreType.DMA
        others = max(nz - 1, 1)
        symbol = pltpu.VMEM((deep * comps, 8, 128), f32)
        tables = (3, comps, comps, stiffness.shape[0])
        flat = (planes * rows * lanes // 128, 128)
        scratch = [pltpu.SMEM((layers,), jnp.int32)]
        scratch += [pltpu.SMEM(tables, f32)] * 2
        scratch += [pltpu.VMEM(flat, f32)] * 2
        scratch += [pltpu.VMEM((tables[3], 2 * 3 * comps * comps, 8, 128), f32), dma((5,))]
        scratch += [pltpu.SMEM((nz, layers), jnp.int32)]
        scratch += [pltpu.VMEM((rows, planes, lanes), f32)] * 2
        scratch += [pltpu.VMEM((n, planes, lanes), f32) for n in (REACH, REACH - 1, REACH, REACH - 1)]
        scratch += [
            pltpu.VMEM((2, planes, packed), f32),
            pltpu.VMEM((2, 3, planes, packed), f32),
            pltpu.VMEM((REACH, rows + 2 * REACH, planes, lanes + 128), f32),
            pltpu.VMEM((REACH - 1, rows + 2 * REACH - 2, planes, lanes + 128), f32),
            pltpu.VMEM((3, planes, lanes + 128), f32),
        ]
        scratch += [symbol] * 6
        scratch += [
            pltpu.VMEM((nz * 2 * planes * 8, 128), f32),
            pltpu.VMEM((3 * nz * 2 * planes, depth), jnp.bfloat16),
            pltpu.VMEM((3, rows, depth, lanes), jnp.bfloat16),
            pltpu.VMEM((rows, 2 * planes, lanes), f32),
            pltpu.VMEM((others, rows, 2 * planes, lanes), f32),
            pltpu.VMEM((others, rows, 2 * planes, lanes), f32),
        ]
        scratch += [dma((nz,))] * 2 + [dma((2, rows // 2, 2))] * 2 + [dma((2, 3))] * 2 + [dma((others, rows))] * 2
        tiled = (layers, comps, rows, lanes // 128, 128)

        def flatten(x):
            return x.reshape(tiled).transpose(0, 1, 3, 2, 4).reshape(-1, 128)

        def unflatten(x):
            split = x.reshape(layers, comps, lanes // 128, rows, 128)
            return split.transpose(0, 1, 3, 2, 4).reshape(dims)

        out = jax.ShapeDtypeStruct(flat, f32)
        given = (layer_material, stiffness.transpose(1, 2, 3, 0), line_factors.transpose(1, 2, 3, 0),
                 flatten(right_side), flatten(start_field))
        given = [pltpu.with_memory_space_constraint(x, pltpu.HBM) for x in given]
        outs = pl.pallas_call(
            functools.partial(kernel, sizes, dims),
            out_shape=(out, out),
            in_specs=[pl.BlockSpec(memory_space=pltpu.HBM)] * 5,
            out_specs=(vmem, vmem),
            scratch_shapes=scratch,
            compiler_params=pltpu.CompilerParams(
                collective_id=0, has_side_effects=True, vmem_limit_bytes=VMEM_LIMIT),
        )(*given)
        return tuple(unflatten(o) for o in outs)

    return jax.shard_map(
        on_device,
        mesh=mesh,
        in_specs=(P("gz", None, "gy", "gx"), P("gz", None, "gy", "gx"), P("gz"), P(), P()),
        out_specs=(P("gz", None, "gy", "gx"), P("gz", None, "gy", "gx")),
        check_vma=False,
    )


VMEM_LIMIT = 40 * 1024 * 1024
```

```python
import functools

import jax
import jax.numpy as jnp
from jax import lax
from jax.experimental import pallas as pl
from jax.experimental.pallas import tpu as pltpu
from jax.sharding import PartitionSpec as P

SWEEPS = 3
REACH = 2 * SWEEPS + 1
POWERS = REACH + 1
SLOT = 8
MESH = pl.DeviceIdType.MESH


def total(terms):
    result = terms[0]
    for term in terms[1:]:
        result = result + term
    return result


def kernel(
    sizes, dims, material_hbm, sten_hbm, fac_hbm, load_hbm, start_hbm, out_u, out_r,
    material, sten, fac, load, start, coef, in_sem,
    mats, own_u, own_b, prev_u, prev_b, next_u, next_b, edge_out, edge_in, work_u, work_b, keep,
    sym_u, sym_b, sym_r, sym_y, sym_e, sym_c, maps, left, right, mine, outgoing, incoming,
    mat_ss, mat_rs, row_ss, row_rs, edge_ss, edge_rs, pass_ss, pass_rs, part_ss, part_rs,
):
    nz, ny, nx = sizes
    layers, comps, rows, lanes = dims
    planes = layers * comps
    deep = nz * layers
    width = lanes + 128
    gz, gy, gx = (lax.axis_index(name) for name in ("gz", "gy", "gx"))
    three = range(comps)
    half_group = -(-planes // 32) * 32
    depth = POWERS * half_group
    pending = []
    fetches = [
        pltpu.make_async_copy(src, dst, in_sem.at[i])
        for i, (src, dst) in enumerate((
            (start_hbm, start), (load_hbm, load), (sten_hbm, sten), (fac_hbm, fac), (material_hbm, material),
        ))
    ]
    for fetch in fetches:
        fetch.start()

    def at(z, y, x):
        return {"gz": z, "gy": y, "gx": x}

    def copy_if(cond, src, dst, ss, rs, target):
        copy = pltpu.make_async_remote_copy(
            src_ref=src, dst_ref=dst, send_sem=ss, recv_sem=rs,
            device_id=target, device_id_type=MESH,
        )

        if cond is True:
            copy.start()
        else:
            @pl.when(cond)
            def _():
                copy.start()

        pending.append((cond, copy))

    def arrive_if(cond, ref, ss, rs):
        copy = pltpu.make_async_remote_copy(
            src_ref=ref, dst_ref=ref, send_sem=ss, recv_sem=rs,
            device_id=at(gz, gy, gx), device_id_type=MESH,
        )
        if cond is True:
            copy.wait_recv()
        else:
            @pl.when(cond)
            def _():
                copy.wait_recv()

    has_prev_y, has_next_y = gy > 0, gy < ny - 1
    has_prev_x, has_next_x = gx > 0, gx < nx - 1
    sides_y = ((-1, has_prev_y), (1, has_next_y))
    sides_x = ((-1, has_prev_x), (1, has_next_x))

    barrier = pltpu.get_barrier_semaphore()
    peers = [(gz != j, at(j, gy, gx)) for j in range(nz)]
    peers += [(cond, at(gz, gy + step, gx)) for step, cond in sides_y]
    peers += [(cond, at(gz, gy, gx + step)) for step, cond in sides_x]
    for cond, target in peers:
        @pl.when(cond)
        def _(target=target):
            pl.semaphore_signal(barrier, inc=1, device_id=target, device_id_type=MESH)

    tiles = lanes // 128
    for own, given, fetch in ((own_u, start, fetches[0]), (own_b, load, fetches[1])):
        fetch.wait()
        for y in range(rows):
            for tile in range(tiles):
                own[y, :, tile * 128 : (tile + 1) * 128] = given[pl.ds(tile * rows + y, planes, stride=tiles * rows), :]

    def place(index):
        return (index * SLOT // 128) * 128, index * SLOT % 128

    tile_lane = lax.broadcasted_iota(jnp.int32, (planes, 128), 1)
    for side in range(2):
        for tile in range(edge_out.shape[2] // 128):
            packed = jnp.zeros((planes, 128), jnp.float32)
            for which, ref in enumerate((own_u, own_b)):
                for y in range(rows):
                    base, spot = place(which * rows + y)
                    if base != tile * 128:
                        continue
                    if side == 0:
                        piece = pltpu.roll(ref[y, :, 0:128], spot, 1) if spot else ref[y, :, 0:128]
                    else:
                        piece = pltpu.roll(ref[y, :, lanes - 128 : lanes], (spot + SLOT) % 128, 1)
                    inside = jnp.logical_and(tile_lane >= spot, tile_lane < spot + SLOT)
                    packed = jnp.where(inside, piece, packed)
            edge_out[side, :, tile * 128 : (tile + 1) * 128] = packed

    fetches[4].wait()
    pl.semaphore_wait(barrier, total([cond.astype(jnp.int32) for cond, _ in peers]))

    for j in range(nz):
        copy_if(gz != j, material, mats.at[gz], mat_ss.at[j], mat_rs.at[gz], at(j, gy, gx))
    strips = ((own_u, prev_u, next_u, REACH), (own_b, prev_b, next_b, REACH - 1))
    stages = rows // 2
    bounds = []
    for which, shared in ((0, 2), (1, 1)):
        reach = strips[which][3]
        enough = max(reach - stages + 1, 0)
        bounds.append(sorted({0, enough}) + list(range(enough + 1, reach + 1)))
    spans = [list(zip(b[:-1], b[1:])) for b in bounds]
    opening = [len([1 for _, last in spans[which] if last <= max(strips[which][3] - stages + 1, 0)]) for which in range(2)]

    def strip(which, step):
        own, prev, after, reach = strips[which]
        first, last = spans[which][step]
        return ((own.at[rows - last : rows - first], prev.at[reach - last : reach - first]),
                (own.at[first:last], after.at[first:last]))

    def send_rows(which, step):
        (out_up, in_up), (out_down, in_down) = strip(which, step)
        copy_if(has_next_y, out_up, in_up,
                row_ss.at[which, step, 0], row_rs.at[which, step, 0], at(gz, gy + 1, gx))
        copy_if(has_prev_y, out_down, in_down,
                row_ss.at[which, step, 1], row_rs.at[which, step, 1], at(gz, gy - 1, gx))

    early = [(0, step) for step in range(opening[0])]
    later = [(1, step) for step in range(opening[1])]
    for more in range(max(len(spans[0]) - opening[0], len(spans[1]) - opening[1])):
        later += [(w, opening[w] + more) for w in range(2) if opening[w] + more < len(spans[w])]
    for side, (step_x, cond_x) in enumerate(sides_x):
        copy_if(cond_x, edge_out.at[side], edge_in.at[1, 1 - side],
                edge_ss.at[1 - side], edge_rs.at[1 - side], at(gz, gy, gx + step_x))

    for which, step in early:
        send_rows(which, step)

    for layer in range(layers):
        mats[gz, layer] = material[layer]
    blocks = 3 * comps * comps
    for fetch in fetches[2:4]:
        fetch.wait()
    for first, table in ((0, sten), (blocks, fac)):
        for which in range(3):
            for i in three:
                for j in three:
                    for mat_id in range(coef.shape[0]):
                        spot = first + (which * comps + i) * comps + j
                        coef[mat_id, spot] = jnp.full((8, 128), table[which, i, j, mat_id], jnp.float32)
    for cond, refs in ((has_prev_y, (prev_u, prev_b)), (has_next_y, (next_u, next_b))):
        @pl.when(jnp.logical_not(cond))
        def _(refs=refs):
            for ref in refs:
                ref[...] = jnp.zeros_like(ref)
    for spot, (step_y, cond_y) in enumerate(sides_y):
        @pl.when(jnp.logical_not(cond_y))
        def _(spot=spot):
            edge_in[2 * spot] = jnp.zeros_like(edge_in[2 * spot])
    for side, (step_x, cond_x) in enumerate(sides_x):
        @pl.when(jnp.logical_not(cond_x))
        def _(side=side):
            edge_in[1, side] = jnp.zeros_like(edge_in[1, side])
    for side, (step_x, cond_x) in enumerate(sides_x):
        arrive_if(cond_x, edge_in.at[1, side], edge_ss.at[side], edge_rs.at[side])
    copy_if(has_next_y, edge_in.at[1], edge_in.at[0], pass_ss.at[0], pass_rs.at[0], at(gz, gy + 1, gx))
    copy_if(has_prev_y, edge_in.at[1], edge_in.at[2], pass_ss.at[1], pass_rs.at[1], at(gz, gy - 1, gx))
    for which, step in later:
        send_rows(which, step)
    wide_lane = lax.broadcasted_iota(jnp.int32, (planes, width), 1)
    inner = (wide_lane < lanes).astype(jnp.float32)
    inner = inner + jnp.where(
        jnp.logical_and(wide_lane >= lanes, wide_lane < lanes + SLOT), has_next_x.astype(jnp.float32), 0.0)
    inner = inner + jnp.where(wide_lane >= width - SLOT, has_prev_x.astype(jnp.float32), 0.0)
    keep[0] = inner * has_prev_y.astype(jnp.float32)
    keep[1] = inner
    keep[2] = inner * has_next_y.astype(jnp.float32)
    for part in range(3):
        for y in range(rows):
            right[part, y, 2 * depth - half_group :, :] = jnp.zeros((half_group, lanes), jnp.bfloat16)

    for j in range(nz):
        arrive_if(gz != j, mats.at[j], mat_ss.at[j], mat_rs.at[j])

    sub = lax.broadcasted_iota(jnp.int32, (8, 128), 0)
    lane = lax.broadcasted_iota(jnp.int32, (8, 128), 1)
    lowest = sub == 0

    def block(table, level, layer, which):
        z = layer * (2 if level else 1)
        mat_id = mats[z // layers, z % layers]
        first = which * comps * comps + (blocks if table is fac else 0)
        return [[coef[mat_id, first + i * comps + j] for j in three] for i in three]

    def times(mat, vec):
        return [total([mat[i][j] * vec[j] for j in three]) for i in three]

    def spread(x):
        return jnp.where(lowest, 0.0, pltpu.roll(x, 1, 0))

    for z in range(deep):
        here = gz == z // layers
        for c in three:
            plane = z % layers * comps + c
            spot = jnp.where(here, plane, -1 - half_group)
            sym_u[z * comps + c] = jnp.logical_and(lowest, lane == spot).astype(jnp.float32)
            sym_b[z * comps + c] = jnp.logical_and(lowest, lane == spot + half_group).astype(jnp.float32)

    def residual(level, field, source, count, layer):
        here = [field[layer * comps + c] for c in three]
        side = [spread(x) for x in here]
        vert = []
        for c in three:
            near = []
            if layer:
                near.append(field[(layer - 1) * comps + c])
            if layer < count - 1:
                near.append(field[(layer + 1) * comps + c])
            vert.append(0.25 * total(near) if level else total(near))
        a = times(block(sten, level, layer, 0), here)
        b = times(block(sten, level, layer, 1), side)
        d = times(block(sten, level, layer, 2), vert)
        return [source[layer * comps + c] - (a[c] - b[c] - d[c]) for c in three]

    def line_solve(level, resid, field, count, fresh):
        carry = None
        for layer in range(count):
            now = times(block(fac, level, layer, 0), resid(layer))
            if carry is not None:
                now = [a + b for a, b in zip(now, times(block(fac, level, layer, 1), carry))]
            for c in three:
                sym_y[layer * comps + c] = now[c]
            carry = now
        back = None
        for layer in reversed(range(count)):
            now = [sym_y[layer * comps + c] for c in three]
            if back is not None:
                now = [a + b for a, b in zip(now, times(block(fac, level, layer, 2), back))]
            for c in three:
                spot = layer * comps + c
                field[spot] = now[c] if fresh else field[spot] + now[c]
            back = now

    for sweep in range(SWEEPS):
        line_solve(0, lambda layer: residual(0, sym_u, sym_b, deep, layer), sym_u, deep, False)
    for k in range(deep // 2):
        pair = [residual(0, sym_u, sym_b, deep, 2 * k + step) for step in range(2)]
        for c in three:
            sym_c[k * comps + c] = pair[0][c] + pair[1][c]
    for sweep in range(SWEEPS):
        if sweep:
            source = functools.partial(residual, 1, sym_e, sym_c, deep // 2)
        else:
            def source(layer):
                return [sym_c[layer * comps + c] for c in three]
        line_solve(1, source, sym_e, deep // 2, sweep == 0)
    for z in range(deep):
        for c in three:
            sym_u[z * comps + c] = sym_u[z * comps + c] + sym_e[z // 2 * comps + c]
    for z in range(deep):
        value = residual(0, sym_u, sym_b, deep, z)
        first = z // layers * 2 * planes + z % layers * comps
        for c in three:
            maps[(first + c) * 8 : (first + c + 1) * 8, :] = sym_u[z * comps + c]
            spot = first + planes + c
            maps[spot * 8 : (spot + 1) * 8, :] = value[c]
    def thirds(x):
        high = x.astype(jnp.bfloat16)
        rest = x - high.astype(jnp.float32)
        middle = rest.astype(jnp.bfloat16)
        return high, middle, (rest - middle.astype(jnp.float32)).astype(jnp.bfloat16)

    size = 2 * planes
    count = nz * size
    map_lane = lax.broadcasted_iota(jnp.int32, (size, 128), 1)
    for i in range(nz):
        target = lax.rem(gz + 1 + i, nz)
        lines = [maps[pl.ds(target * size * 8 + power, size, stride=8), :] for power in range(POWERS)]
        for which in range(2):
            base = which * half_group
            inside = jnp.logical_and(map_lane >= base, map_lane < base + half_group)
            each = 128 // half_group
            for tile in range(POWERS // each):
                value = jnp.zeros((size, 128), jnp.float32)
                for part in range(each):
                    piece = jnp.where(inside, lines[tile * each + part], 0.0)
                    shift = (part * half_group - base) % 128
                    value = value + (pltpu.roll(piece, shift, 1) if shift else piece)
                first = which * depth + tile * 128
                for part, third in enumerate(thirds(value)):
                    left[part * count + i * size : part * count + (i + 1) * size, first : first + 128] = third

    def raw(which, y):
        own, prev, after, reach = strips[which]
        if y < 0:
            middle, step_y, line = prev[reach + y], -1, rows + y
        elif y < rows:
            middle, step_y, line = own[y], 0, y
        else:
            middle, step_y, line = after[y - rows], 1, y - rows
        base, spot = place(which * rows + line)
        west = pltpu.roll(edge_in[1 + step_y, 0, :, base : base + 128], (128 - SLOT - spot) % 128, 1)
        east = edge_in[1 + step_y, 1, :, base : base + 128]
        if spot:
            east = pltpu.roll(east, 128 - spot, 1)
        tail = jnp.where(tile_lane < SLOT, east, jnp.where(tile_lane >= 128 - SLOT, west, 0.0))
        return jnp.concatenate([middle, tail], axis=1)

    padding = jnp.zeros((half_group - planes, lanes), jnp.float32)
    done = set()

    def extend(which, known_rows):
        work, reach = (work_u, work_b)[which], strips[which][3]
        for power in range(reach + 1):
            for y in range(power - known_rows, rows + known_rows - power):
                if (which, power, y) in done:
                    continue
                done.add((which, power, y))
                if power == 0:
                    value = raw(which, y)
                else:
                    x = work[power - 1, y + reach]
                    value = pltpu.roll(x, 1, 1) + pltpu.roll(x, width - 1, 1)
                    value = value + (work[power - 1, y + reach - 1] + work[power - 1, y + reach + 1])
                    value = value * keep[0 if y < 0 else 1 if y < rows else 2]
                if power < reach:
                    work[power, y + reach] = value
                if 0 <= y < rows:
                    first = which * depth + power * half_group
                    cell = value[:, :lanes]
                    if half_group > planes:
                        cell = jnp.concatenate([cell, padding], axis=0)
                    for part, third in enumerate(thirds(cell)):
                        right[part, y, first : first + half_group, :] = third

    def take(which, step):
        (_, in_up), (_, in_down) = strip(which, step)
        arrive_if(has_prev_y, in_up, row_ss.at[which, step, 0], row_rs.at[which, step, 0])
        arrive_if(has_next_y, in_down, row_ss.at[which, step, 1], row_rs.at[which, step, 1])
        extend(which, spans[which][step][1])

    for which in range(2):
        extend(which, 0)
    for spot, (step_y, cond_y) in enumerate(sides_y):
        arrive_if(cond_y, edge_in.at[2 * spot], pass_ss.at[spot], pass_rs.at[spot])
    for stage in range(stages):
        for which in range(2):
            first = opening[which] + stage - 1 if stage else 0
            for step in range(first, opening[which] + stage):
                if step < len(spans[which]):
                    take(which, step)
        for y in (stages - 1 - stage, stages + stage):
            pieces = []
            for part in (2, 1, 0):
                product = jnp.dot(left[: (3 - part) * count], right[part, y], preferred_element_type=jnp.float32)
                pieces += [product[k * count : (k + 1) * count] for k in reversed(range(3 - part))]
            value = total(pieces)
            for i in range(nz - 1):
                outgoing[i, y] = value[i * size : (i + 1) * size]
                copy_if(True, outgoing.at[i, y], incoming.at[i, y],
                        part_ss.at[i, y], part_rs.at[i, y], at(lax.rem(gz + 1 + i, nz), gy, gx))
            mine[y] = value[(nz - 1) * size :]
    for y in [y for stage in range(stages) for y in (stages - 1 - stage, stages + stage)]:
        value = mine[y]
        for i in range(nz - 1):
            arrive_if(True, incoming.at[i, y], part_ss.at[i, y], part_rs.at[i, y])
            value = value + incoming[i, y]
        for tile in range(tiles):
            part = value[:, tile * 128 : (tile + 1) * 128]
            spots = pl.ds(tile * rows + y, planes, stride=tiles * rows)
            out_u[spots, :] = part[:planes]
            out_r[spots, :] = part[planes:]
    for cond, copy in pending:
        if cond is True:
            copy.wait_send()
        else:
            @pl.when(cond)
            def _(copy=copy):
                copy.wait_send()


def put(from_u, from_r, to_u, to_r, sem):
    copies = [pltpu.make_async_copy(src, dst, sem.at[i]) for i, (src, dst) in enumerate(((from_u, to_u), (from_r, to_r)))]
    for copy in copies:
        copy.start()
    for copy in copies:
        copy.wait()


def solution(mesh):
    sizes = tuple(mesh.shape[name] for name in ("gz", "gy", "gx"))
    nz = sizes[0]

    def on_device(right_side, start_field, layer_material, stiffness, line_factors):
        dims = right_side.shape
        layers, comps, rows, lanes = dims
        planes = layers * comps
        deep = nz * layers
        half_group = -(-planes // 32) * 32
        depth = POWERS * 2 * half_group
        packed = -(-2 * rows * SLOT // 128) * 128
        f32 = jnp.float32
        vmem = pl.BlockSpec(memory_space=pltpu.VMEM)
        dma = pltpu.SemaphoreType.DMA
        others = max(nz - 1, 1)
        symbol = pltpu.VMEM((deep * comps, 8, 128), f32)
        tables = (3, comps, comps, stiffness.shape[0])
        flat = (planes * rows * lanes // 128, 128)
        scratch = [pltpu.SMEM((layers,), jnp.int32)]
        scratch += [pltpu.SMEM(tables, f32)] * 2
        scratch += [pltpu.VMEM(flat, f32)] * 2
        scratch += [pltpu.VMEM((tables[3], 2 * 3 * comps * comps, 8, 128), f32), dma((5,))]
        scratch += [pltpu.SMEM((nz, layers), jnp.int32)]
        scratch += [pltpu.VMEM((rows, planes, lanes), f32)] * 2
        scratch += [pltpu.VMEM((n, planes, lanes), f32) for n in (REACH, REACH - 1, REACH, REACH - 1)]
        scratch += [
            pltpu.VMEM((2, planes, packed), f32),
            pltpu.VMEM((3, 2, planes, packed), f32),
            pltpu.VMEM((REACH, rows + 2 * REACH, planes, lanes + 128), f32),
            pltpu.VMEM((REACH - 1, rows + 2 * REACH - 2, planes, lanes + 128), f32),
            pltpu.VMEM((3, planes, lanes + 128), f32),
        ]
        scratch += [symbol] * 6
        scratch += [
            pltpu.VMEM((nz * 2 * planes * 8, 128), f32),
            pltpu.VMEM((3 * nz * 2 * planes, depth), jnp.bfloat16),
            pltpu.VMEM((3, rows, depth, lanes), jnp.bfloat16),
            pltpu.VMEM((rows, 2 * planes, lanes), f32),
            pltpu.VMEM((others, rows, 2 * planes, lanes), f32),
            pltpu.VMEM((others, rows, 2 * planes, lanes), f32),
        ]
        scratch += [dma((nz,))] * 2 + [dma((2, REACH, 2))] * 2 + [dma((2,))] * 4 + [dma((others, rows))] * 2
        tiled = (layers, comps, rows, lanes // 128, 128)

        def flatten(x):
            return x.reshape(tiled).transpose(0, 1, 3, 2, 4).reshape(-1, 128)

        def unflatten(x):
            split = x.reshape(layers, comps, lanes // 128, rows, 128)
            return split.transpose(0, 1, 3, 2, 4).reshape(dims)

        out = jax.ShapeDtypeStruct(flat, f32)
        given = (layer_material, stiffness.transpose(1, 2, 3, 0), line_factors.transpose(1, 2, 3, 0),
                 flatten(right_side), flatten(start_field))
        given = [pltpu.with_memory_space_constraint(x, pltpu.HBM) for x in given]
        outs = pl.pallas_call(
            functools.partial(kernel, sizes, dims),
            out_shape=(out, out),
            in_specs=[pl.BlockSpec(memory_space=pltpu.HBM)] * 5,
            out_specs=(vmem, vmem),
            scratch_shapes=scratch,
            compiler_params=pltpu.CompilerParams(
                collective_id=0, has_side_effects=True, vmem_limit_bytes=VMEM_LIMIT),
        )(*given)
        outs = pl.pallas_call(
            put,
            out_shape=(out, out),
            in_specs=[vmem, vmem],
            out_specs=(pl.BlockSpec(memory_space=pltpu.HBM),) * 2,
            scratch_shapes=[dma((2,))],
            compiler_params=pltpu.CompilerParams(vmem_limit_bytes=4 * 1024 * 1024),
        )(*outs)
        return tuple(unflatten(o) for o in outs)

    return jax.shard_map(
        on_device,
        mesh=mesh,
        in_specs=(P("gz", None, "gy", "gx"), P("gz", None, "gy", "gx"), P("gz"), P(), P()),
        out_specs=(P("gz", None, "gy", "gx"), P("gz", None, "gy", "gx")),
        check_vma=False,
    )


VMEM_LIMIT = 40 * 1024 * 1024
```

```python
import functools

import jax
import jax.numpy as jnp
from jax import lax
from jax.experimental import pallas as pl
from jax.experimental.pallas import tpu as pltpu
from jax.sharding import PartitionSpec as P

SWEEPS = 3
REACH = 2 * SWEEPS + 1
POWERS = REACH + 1
SLOT = 8
MESH = pl.DeviceIdType.MESH


def total(terms):
    result = terms[0]
    for term in terms[1:]:
        result = result + term
    return result


def kernel(
    sizes, dims, material_hbm, sten_hbm, fac_hbm, load_hbm, start_hbm, out_u, out_r,
    material, sten, fac, load, start, coef, in_sem,
    mats, own_u, own_b, prev_u, prev_b, next_u, next_b, edge_out, edge_in, work_u, work_b, keep,
    sym_u, sym_b, sym_r, sym_y, sym_e, sym_c, maps, left, right, mine, outgoing, incoming, rim_out, rim_in, side_out, side_in,
    mat_ss, mat_rs, row_ss, row_rs, edge_ss, edge_rs, pass_ss, pass_rs, part_ss, part_rs, rim_ss, rim_rs, side_ss, side_rs,
):
    nz, ny, nx = sizes
    layers, comps, rows, lanes = dims
    planes = layers * comps
    deep = nz * layers
    width = lanes + 128
    gz, gy, gx = (lax.axis_index(name) for name in ("gz", "gy", "gx"))
    three = range(comps)
    half_group = -(-planes // 32) * 32
    depth = POWERS * half_group
    pending = []
    fetches = [
        pltpu.make_async_copy(src, dst, in_sem.at[i])
        for i, (src, dst) in enumerate((
            (start_hbm, start), (load_hbm, load), (sten_hbm, sten), (fac_hbm, fac), (material_hbm, material),
        ))
    ]
    for fetch in fetches:
        fetch.start()

    def at(z, y, x):
        return {"gz": z, "gy": y, "gx": x}

    def copy_if(cond, src, dst, ss, rs, target):
        copy = pltpu.make_async_remote_copy(
            src_ref=src, dst_ref=dst, send_sem=ss, recv_sem=rs,
            device_id=target, device_id_type=MESH,
        )

        if cond is True:
            copy.start()
        else:
            @pl.when(cond)
            def _():
                copy.start()

        pending.append((cond, copy))

    def arrive_if(cond, ref, ss, rs):
        copy = pltpu.make_async_remote_copy(
            src_ref=ref, dst_ref=ref, send_sem=ss, recv_sem=rs,
            device_id=at(gz, gy, gx), device_id_type=MESH,
        )
        if cond is True:
            copy.wait_recv()
        else:
            @pl.when(cond)
            def _():
                copy.wait_recv()

    has_prev_y, has_next_y = gy > 0, gy < ny - 1
    has_prev_x, has_next_x = gx > 0, gx < nx - 1
    sides_y = ((-1, has_prev_y), (1, has_next_y))
    sides_x = ((-1, has_prev_x), (1, has_next_x))

    barrier = pltpu.get_barrier_semaphore()
    peers = [(gz != j, at(j, gy, gx)) for j in range(nz)]
    peers += [(cond, at(gz, gy + step, gx)) for step, cond in sides_y]
    peers += [(cond, at(gz, gy, gx + step)) for step, cond in sides_x]
    for cond, target in peers:
        @pl.when(cond)
        def _(target=target):
            pl.semaphore_signal(barrier, inc=1, device_id=target, device_id_type=MESH)

    tiles = lanes // 128
    for own, given, fetch in ((own_u, start, fetches[0]), (own_b, load, fetches[1])):
        fetch.wait()
        for y in range(rows):
            for tile in range(tiles):
                own[y, :, tile * 128 : (tile + 1) * 128] = given[pl.ds(tile * rows + y, planes, stride=tiles * rows), :]

    def place(index):
        return (index * SLOT // 128) * 128, index * SLOT % 128

    tile_lane = lax.broadcasted_iota(jnp.int32, (planes, 128), 1)
    for side in range(2):
        for tile in range(edge_out.shape[2] // 128):
            packed = jnp.zeros((planes, 128), jnp.float32)
            for which, ref in enumerate((own_u, own_b)):
                for y in range(rows):
                    base, spot = place(which * rows + y)
                    if base != tile * 128:
                        continue
                    if side == 0:
                        piece = pltpu.roll(ref[y, :, 0:128], spot, 1) if spot else ref[y, :, 0:128]
                    else:
                        piece = pltpu.roll(ref[y, :, lanes - 128 : lanes], (spot + SLOT) % 128, 1)
                    inside = jnp.logical_and(tile_lane >= spot, tile_lane < spot + SLOT)
                    packed = jnp.where(inside, piece, packed)
            edge_out[side, :, tile * 128 : (tile + 1) * 128] = packed

    fetches[4].wait()
    pl.semaphore_wait(barrier, total([cond.astype(jnp.int32) for cond, _ in peers]))

    for j in range(nz):
        copy_if(gz != j, material, mats.at[gz], mat_ss.at[j], mat_rs.at[gz], at(j, gy, gx))
    strips = ((own_u, prev_u, next_u, REACH), (own_b, prev_b, next_b, REACH - 1))
    stages = rows // 2
    bounds = []
    for which, shared in ((0, 2), (1, 1)):
        reach = strips[which][3]
        enough = max(reach - stages + 1, 0)
        bounds.append(sorted({0, enough}) + list(range(enough + 1, reach + 1)))
    spans = [list(zip(b[:-1], b[1:])) for b in bounds]
    opening = [len([1 for _, last in spans[which] if last <= max(strips[which][3] - stages + 1, 0)]) for which in range(2)]

    def strip(which, step):
        own, prev, after, reach = strips[which]
        first, last = spans[which][step]
        return ((own.at[rows - last : rows - first], prev.at[reach - last : reach - first]),
                (own.at[first:last], after.at[first:last]))

    def send_rows(which, step):
        (out_up, in_up), (out_down, in_down) = strip(which, step)
        copy_if(has_next_y, out_up, in_up,
                row_ss.at[which, step, 0], row_rs.at[which, step, 0], at(gz, gy + 1, gx))
        copy_if(has_prev_y, out_down, in_down,
                row_ss.at[which, step, 1], row_rs.at[which, step, 1], at(gz, gy - 1, gx))

    early = [(0, step) for step in range(opening[0])]
    later = [(1, step) for step in range(opening[1])]
    for more in range(max(len(spans[0]) - opening[0], len(spans[1]) - opening[1])):
        later += [(w, opening[w] + more) for w in range(2) if opening[w] + more < len(spans[w])]
    for side, (step_x, cond_x) in enumerate(sides_x):
        copy_if(cond_x, edge_out.at[side], edge_in.at[1, 1 - side],
                edge_ss.at[1 - side], edge_rs.at[1 - side], at(gz, gy, gx + step_x))

    for which, step in early:
        send_rows(which, step)

    for layer in range(layers):
        mats[gz, layer] = material[layer]
    blocks = 3 * comps * comps
    for fetch in fetches[2:4]:
        fetch.wait()
    for first, table in ((0, sten), (blocks, fac)):
        for which in range(3):
            for i in three:
                for j in three:
                    for mat_id in range(coef.shape[0]):
                        spot = first + (which * comps + i) * comps + j
                        coef[mat_id, spot] = jnp.full((8, 128), table[which, i, j, mat_id], jnp.float32)
    for cond, refs in ((has_prev_y, (prev_u, prev_b)), (has_next_y, (next_u, next_b))):
        @pl.when(jnp.logical_not(cond))
        def _(refs=refs):
            for ref in refs:
                ref[...] = jnp.zeros_like(ref)
    for spot, (step_y, cond_y) in enumerate(sides_y):
        @pl.when(jnp.logical_not(cond_y))
        def _(spot=spot):
            edge_in[2 * spot] = jnp.zeros_like(edge_in[2 * spot])
    for side, (step_x, cond_x) in enumerate(sides_x):
        @pl.when(jnp.logical_not(cond_x))
        def _(side=side):
            edge_in[1, side] = jnp.zeros_like(edge_in[1, side])
    for side, (step_x, cond_x) in enumerate(sides_x):
        arrive_if(cond_x, edge_in.at[1, side], edge_ss.at[side], edge_rs.at[side])
    copy_if(has_next_y, edge_in.at[1], edge_in.at[0], pass_ss.at[0], pass_rs.at[0], at(gz, gy + 1, gx))
    copy_if(has_prev_y, edge_in.at[1], edge_in.at[2], pass_ss.at[1], pass_rs.at[1], at(gz, gy - 1, gx))
    for which, step in later:
        send_rows(which, step)
    wide_lane = lax.broadcasted_iota(jnp.int32, (planes, width), 1)
    inner = (wide_lane < lanes).astype(jnp.float32)
    inner = inner + jnp.where(
        jnp.logical_and(wide_lane >= lanes, wide_lane < lanes + SLOT), has_next_x.astype(jnp.float32), 0.0)
    inner = inner + jnp.where(wide_lane >= width - SLOT, has_prev_x.astype(jnp.float32), 0.0)
    keep[0] = inner * has_prev_y.astype(jnp.float32)
    keep[1] = inner
    keep[2] = inner * has_next_y.astype(jnp.float32)
    for part in range(3):
        for y in range(rows):
            right[part, y, 2 * depth - half_group :, :] = jnp.zeros((half_group, lanes), jnp.bfloat16)

    for j in range(nz):
        arrive_if(gz != j, mats.at[j], mat_ss.at[j], mat_rs.at[j])

    sub = lax.broadcasted_iota(jnp.int32, (8, 128), 0)
    lane = lax.broadcasted_iota(jnp.int32, (8, 128), 1)
    lowest = sub == 0

    def block(table, level, layer, which):
        z = layer * (2 if level else 1)
        mat_id = mats[z // layers, z % layers]
        first = which * comps * comps + (blocks if table is fac else 0)
        return [[coef[mat_id, first + i * comps + j] for j in three] for i in three]

    def times(mat, vec):
        return [total([mat[i][j] * vec[j] for j in three]) for i in three]

    def spread(x):
        return jnp.where(lowest, 0.0, pltpu.roll(x, 1, 0))

    for z in range(deep):
        here = gz == z // layers
        for c in three:
            plane = z % layers * comps + c
            spot = jnp.where(here, plane, -1 - half_group)
            sym_u[z * comps + c] = jnp.logical_and(lowest, lane == spot).astype(jnp.float32)
            sym_b[z * comps + c] = jnp.logical_and(lowest, lane == spot + half_group).astype(jnp.float32)

    def residual(level, field, source, count, layer):
        here = [field[layer * comps + c] for c in three]
        side = [spread(x) for x in here]
        vert = []
        for c in three:
            near = []
            if layer:
                near.append(field[(layer - 1) * comps + c])
            if layer < count - 1:
                near.append(field[(layer + 1) * comps + c])
            vert.append(0.25 * total(near) if level else total(near))
        a = times(block(sten, level, layer, 0), here)
        b = times(block(sten, level, layer, 1), side)
        d = times(block(sten, level, layer, 2), vert)
        return [source[layer * comps + c] - (a[c] - b[c] - d[c]) for c in three]

    def line_solve(level, resid, field, count, fresh):
        carry = None
        for layer in range(count):
            now = times(block(fac, level, layer, 0), resid(layer))
            if carry is not None:
                now = [a + b for a, b in zip(now, times(block(fac, level, layer, 1), carry))]
            for c in three:
                sym_y[layer * comps + c] = now[c]
            carry = now
        back = None
        for layer in reversed(range(count)):
            now = [sym_y[layer * comps + c] for c in three]
            if back is not None:
                now = [a + b for a, b in zip(now, times(block(fac, level, layer, 2), back))]
            for c in three:
                spot = layer * comps + c
                field[spot] = now[c] if fresh else field[spot] + now[c]
            back = now

    for sweep in range(SWEEPS):
        line_solve(0, lambda layer: residual(0, sym_u, sym_b, deep, layer), sym_u, deep, False)
    for k in range(deep // 2):
        pair = [residual(0, sym_u, sym_b, deep, 2 * k + step) for step in range(2)]
        for c in three:
            sym_c[k * comps + c] = pair[0][c] + pair[1][c]
    for sweep in range(SWEEPS):
        if sweep:
            source = functools.partial(residual, 1, sym_e, sym_c, deep // 2)
        else:
            def source(layer):
                return [sym_c[layer * comps + c] for c in three]
        line_solve(1, source, sym_e, deep // 2, sweep == 0)
    for z in range(deep):
        for c in three:
            sym_u[z * comps + c] = sym_u[z * comps + c] + sym_e[z // 2 * comps + c]
    for z in range(deep):
        value = residual(0, sym_u, sym_b, deep, z)
        first = z // layers * 2 * planes + z % layers * comps
        for c in three:
            maps[(first + c) * 8 : (first + c + 1) * 8, :] = sym_u[z * comps + c]
            spot = first + planes + c
            maps[spot * 8 : (spot + 1) * 8, :] = value[c]
    def thirds(x):
        high = x.astype(jnp.bfloat16)
        rest = x - high.astype(jnp.float32)
        middle = rest.astype(jnp.bfloat16)
        return high, middle, (rest - middle.astype(jnp.float32)).astype(jnp.bfloat16)

    size = 2 * planes
    count = nz * size
    map_lane = lax.broadcasted_iota(jnp.int32, (size, 128), 1)
    for i in range(nz):
        target = lax.rem(gz + 1 + i, nz)
        lines = [maps[pl.ds(target * size * 8 + power, size, stride=8), :] for power in range(POWERS)]
        for which in range(2):
            base = which * half_group
            inside = jnp.logical_and(map_lane >= base, map_lane < base + half_group)
            each = 128 // half_group
            for tile in range(POWERS // each):
                value = jnp.zeros((size, 128), jnp.float32)
                for part in range(each):
                    piece = jnp.where(inside, lines[tile * each + part], 0.0)
                    shift = (part * half_group - base) % 128
                    value = value + (pltpu.roll(piece, shift, 1) if shift else piece)
                first = which * depth + tile * 128
                for part, third in enumerate(thirds(value)):
                    left[part * count + i * size : part * count + (i + 1) * size, first : first + 128] = third

    def raw(which, y):
        own, prev, after, reach = strips[which]
        if y < 0:
            middle, step_y, line = prev[reach + y], -1, rows + y
        elif y < rows:
            middle, step_y, line = own[y], 0, y
        else:
            middle, step_y, line = after[y - rows], 1, y - rows
        base, spot = place(which * rows + line)
        west = pltpu.roll(edge_in[1 + step_y, 0, :, base : base + 128], (128 - SLOT - spot) % 128, 1)
        east = edge_in[1 + step_y, 1, :, base : base + 128]
        if spot:
            east = pltpu.roll(east, 128 - spot, 1)
        tail = jnp.where(tile_lane < SLOT, east, jnp.where(tile_lane >= 128 - SLOT, west, 0.0))
        return jnp.concatenate([middle, tail], axis=1)

    padding = jnp.zeros((half_group - planes, lanes), jnp.float32)
    done = set()

    def extend(which, known_rows):
        work, reach = (work_u, work_b)[which], strips[which][3]
        for power in range(reach + 1):
            for y in range(power - known_rows, rows + known_rows - power):
                if (which, power, y) in done:
                    continue
                done.add((which, power, y))
                if power == 0:
                    value = raw(which, y)
                else:
                    x = work[power - 1, y + reach]
                    value = pltpu.roll(x, 1, 1) + pltpu.roll(x, width - 1, 1)
                    value = value + (work[power - 1, y + reach - 1] + work[power - 1, y + reach + 1])
                    value = value * keep[0 if y < 0 else 1 if y < rows else 2]
                if power < reach:
                    work[power, y + reach] = value
                if 0 <= y < rows:
                    first = which * depth + power * half_group
                    cell = value[:, :lanes]
                    if half_group > planes:
                        cell = jnp.concatenate([cell, padding], axis=0)
                    for part, third in enumerate(thirds(cell)):
                        right[part, y, first : first + half_group, :] = third

    def take(which, step):
        (_, in_up), (_, in_down) = strip(which, step)
        arrive_if(has_prev_y, in_up, row_ss.at[which, step, 0], row_rs.at[which, step, 0])
        arrive_if(has_next_y, in_down, row_ss.at[which, step, 1], row_rs.at[which, step, 1])
        extend(which, spans[which][step][1])

    for which in range(2):
        extend(which, 0)
    for spot, (step_y, cond_y) in enumerate(sides_y):
        arrive_if(cond_y, edge_in.at[2 * spot], pass_ss.at[spot], pass_rs.at[spot])
    rim_id = lax.broadcasted_iota(jnp.int32, (8, lanes), 0)
    rim_low, rim_high = rim_id < comps, rim_id >= 8 - comps
    columns = [jnp.zeros((planes, 128), jnp.float32)] * (nz - 1)

    def side_tile(field, y):
        first = jnp.where(tile_lane == 2 * y, pltpu.roll(field[:, :128], 2 * y, 1), 0.0)
        last = jnp.where(tile_lane == 2 * y + 1, pltpu.roll(field[:, lanes - 128 :], (2 * y + 2) % 128, 1), 0.0)
        return first + last

    for stage in range(stages):
        for which in range(2):
            first = opening[which] + stage - 1 if stage else 0
            for step in range(first, opening[which] + stage):
                if step < len(spans[which]):
                    take(which, step)
        for y in (stages - 1 - stage, stages + stage):
            pieces = []
            for part in (2, 1, 0):
                product = jnp.dot(left[: (3 - part) * count], right[part, y], preferred_element_type=jnp.float32)
                pieces += [product[k * count : (k + 1) * count] for k in reversed(range(3 - part))]
            value = total(pieces)
            for i in range(nz - 1):
                target = at(lax.rem(gz + 1 + i, nz), gy, gx)
                share = value[i * size : (i + 1) * size]
                whole = y in (0, rows - 1)
                outgoing[i, y] = share
                amount = size if whole else planes
                copy_if(True, outgoing.at[i, y, 0:amount], incoming.at[i, y, 0:amount],
                        part_ss.at[i, y], part_rs.at[i, y], target)
                if whole:
                    continue
                ends = share[planes : planes + 8], share[size - 8 : size]
                rim_out[i, y] = jnp.where(rim_low, ends[0], ends[1])
                copy_if(True, rim_out.at[i, y], rim_in.at[i, y], rim_ss.at[i, y], rim_rs.at[i, y], target)
                columns[i] = columns[i] + side_tile(share[planes:], y)
                if stage == stages - 2 and y == stages + stage:
                    side_out[i] = columns[i]
                    copy_if(True, side_out.at[i], side_in.at[i], side_ss.at[i], side_rs.at[i], target)
            mine[y] = value[(nz - 1) * size :]
    rest_id = lax.broadcasted_iota(jnp.int32, (planes, 128), 0)
    for y in [y for stage in range(stages) for y in (stages - 1 - stage, stages + stage)]:
        value = mine[y]
        whole = y in (0, rows - 1)
        solved, rest = value[:planes], value[planes:]
        for i in range(nz - 1):
            amount = size if whole else planes
            arrive_if(True, incoming.at[i, y, 0:amount], part_ss.at[i, y], part_rs.at[i, y])
            solved = solved + incoming[i, y, 0:planes]
            if whole:
                rest = rest + incoming[i, y, planes:size]
        for tile in range(tiles):
            spots = pl.ds(tile * rows + y, planes, stride=tiles * rows)
            out_u[spots, :] = solved[:, tile * 128 : (tile + 1) * 128]
            if whole:
                out_r[spots, :] = rest[:, tile * 128 : (tile + 1) * 128]
        if y == 1:
            for i in range(nz - 1):
                arrive_if(True, side_in.at[i], side_ss.at[i], side_rs.at[i])
        if y == rows - 2:
            sides = total([side_in[i] for i in range(nz - 1)]) if nz > 1 else jnp.zeros((planes, 128), jnp.float32)
            for line in range(1, rows - 1):
                rest = mine[line][planes:]
                ends = jnp.zeros((8, lanes), jnp.float32)
                for i in range(nz - 1):
                    arrive_if(True, rim_in.at[i, line], rim_ss.at[i, line], rim_rs.at[i, line])
                    ends = ends + rim_in[i, line]
                ends = [jnp.where(rim_low, ends, 0.0), jnp.where(rim_high, ends, 0.0)]
                cut = [rest[:8] + ends[0], rest[8 : planes - 8], rest[planes - 8 :] + ends[1]]
                rest = jnp.concatenate(cut, axis=0)
                inner_side = jnp.logical_and(rest_id >= comps, rest_id < planes - comps)
                for tile in range(tiles):
                    part = rest[:, tile * 128 : (tile + 1) * 128]
                    if tile == 0:
                        add = pltpu.roll(sides, 128 - 2 * line, 1)
                        part = part + jnp.where(jnp.logical_and(inner_side, tile_lane == 0), add, 0.0)
                    if tile == tiles - 1:
                        add = pltpu.roll(sides, 126 - 2 * line, 1)
                        part = part + jnp.where(jnp.logical_and(inner_side, tile_lane == 127), add, 0.0)
                    out_r[pl.ds(tile * rows + line, planes, stride=tiles * rows), :] = part

    row_id = lax.broadcasted_iota(jnp.int32, (rows, 128), 0)
    lane_id = lax.broadcasted_iota(jnp.int32, (rows, 128), 1)
    row_rim = jnp.logical_or(row_id == 0, row_id == rows - 1)

    def solution_tile(layer, c, tile):
        first = ((layer * comps + c) * tiles + tile) * rows
        return pl.ds(first, rows)

    def shares(layer, first):
        mat_id = mats[gz, layer]
        return [[coef[mat_id, first + i * comps + j] for j in three] for i in three]

    for layer in range(1, layers - 1):
        mat = [shares(layer, which * comps * comps) for which in range(3)]
        for tile in range(tiles):
            here, side, vert = [], [], []
            for c in three:
                x = out_u[solution_tile(layer, c, tile), :]
                west = out_u[solution_tile(layer, c, tile - 1), :] if tile else x
                east = out_u[solution_tile(layer, c, tile + 1), :] if tile < tiles - 1 else x
                beside = jnp.where(lane_id == 127, west, x), jnp.where(lane_id == 0, east, x)
                around = pltpu.roll(beside[0], 1, 1) + pltpu.roll(beside[1], 127, 1)
                here.append(x)
                side.append(around + (pltpu.roll(x, 1, 0) + pltpu.roll(x, rows - 1, 0)))
                vert.append(out_u[solution_tile(layer - 1, c, tile), :] + out_u[solution_tile(layer + 1, c, tile), :])
            a, b, d = (times(mat[which], vec) for which, vec in enumerate((here, side, vert)))
            rim = row_rim
            if tile == 0:
                rim = jnp.logical_or(rim, lane_id == 0)
            if tile == tiles - 1:
                rim = jnp.logical_or(rim, lane_id == 127)
            for c in three:
                spot = solution_tile(layer, c, tile)
                first = ((layer * comps + c) * tiles + tile) * rows
                value = load[first : first + rows, :] - (a[c] - b[c] - d[c])
                out_r[spot, :] = jnp.where(rim, out_r[spot, :], value)
    for cond, copy in pending:
        if cond is True:
            copy.wait_send()
        else:
            @pl.when(cond)
            def _(copy=copy):
                copy.wait_send()


def put(from_u, from_r, to_u, to_r, sem):
    copies = [pltpu.make_async_copy(src, dst, sem.at[i]) for i, (src, dst) in enumerate(((from_u, to_u), (from_r, to_r)))]
    for copy in copies:
        copy.start()
    for copy in copies:
        copy.wait()


def solution(mesh):
    sizes = tuple(mesh.shape[name] for name in ("gz", "gy", "gx"))
    nz = sizes[0]

    def on_device(right_side, start_field, layer_material, stiffness, line_factors):
        dims = right_side.shape
        layers, comps, rows, lanes = dims
        planes = layers * comps
        deep = nz * layers
        half_group = -(-planes // 32) * 32
        depth = POWERS * 2 * half_group
        packed = -(-2 * rows * SLOT // 128) * 128
        f32 = jnp.float32
        vmem = pl.BlockSpec(memory_space=pltpu.VMEM)
        dma = pltpu.SemaphoreType.DMA
        others = max(nz - 1, 1)
        symbol = pltpu.VMEM((deep * comps, 8, 128), f32)
        tables = (3, comps, comps, stiffness.shape[0])
        flat = (planes * rows * lanes // 128, 128)
        scratch = [pltpu.SMEM((layers,), jnp.int32)]
        scratch += [pltpu.SMEM(tables, f32)] * 2
        scratch += [pltpu.VMEM(flat, f32)] * 2
        scratch += [pltpu.VMEM((tables[3], 2 * 3 * comps * comps, 8, 128), f32), dma((5,))]
        scratch += [pltpu.SMEM((nz, layers), jnp.int32)]
        scratch += [pltpu.VMEM((rows, planes, lanes), f32)] * 2
        scratch += [pltpu.VMEM((n, planes, lanes), f32) for n in (REACH, REACH - 1, REACH, REACH - 1)]
        scratch += [
            pltpu.VMEM((2, planes, packed), f32),
            pltpu.VMEM((3, 2, planes, packed), f32),
            pltpu.VMEM((REACH, rows + 2 * REACH, planes, lanes + 128), f32),
            pltpu.VMEM((REACH - 1, rows + 2 * REACH - 2, planes, lanes + 128), f32),
            pltpu.VMEM((3, planes, lanes + 128), f32),
        ]
        scratch += [symbol] * 6
        scratch += [
            pltpu.VMEM((nz * 2 * planes * 8, 128), f32),
            pltpu.VMEM((3 * nz * 2 * planes, depth), jnp.bfloat16),
            pltpu.VMEM((3, rows, depth, lanes), jnp.bfloat16),
            pltpu.VMEM((rows, 2 * planes, lanes), f32),
            pltpu.VMEM((others, rows, 2 * planes, lanes), f32),
            pltpu.VMEM((others, rows, 2 * planes, lanes), f32),
        ]
        scratch += [pltpu.VMEM((others, rows, 8, lanes), f32)] * 2 + [pltpu.VMEM((others, planes, 128), f32)] * 2
        scratch += [dma((nz,))] * 2 + [dma((2, REACH, 2))] * 2 + [dma((2,))] * 4 + [dma((others, rows))] * 4 + [dma((others,))] * 2
        tiled = (layers, comps, rows, lanes // 128, 128)

        def flatten(x):
            return x.reshape(tiled).transpose(0, 1, 3, 2, 4).reshape(-1, 128)

        def unflatten(x):
            split = x.reshape(layers, comps, lanes // 128, rows, 128)
            return split.transpose(0, 1, 3, 2, 4).reshape(dims)

        out = jax.ShapeDtypeStruct(flat, f32)
        given = (layer_material, stiffness.transpose(1, 2, 3, 0), line_factors.transpose(1, 2, 3, 0),
                 flatten(right_side), flatten(start_field))
        given = [pltpu.with_memory_space_constraint(x, pltpu.HBM) for x in given]
        outs = pl.pallas_call(
            functools.partial(kernel, sizes, dims),
            out_shape=(out, out),
            in_specs=[pl.BlockSpec(memory_space=pltpu.HBM)] * 5,
            out_specs=(vmem, vmem),
            scratch_shapes=scratch,
            compiler_params=pltpu.CompilerParams(
                collective_id=0, has_side_effects=True, vmem_limit_bytes=VMEM_LIMIT),
        )(*given)
        outs = pl.pallas_call(
            put,
            out_shape=(out, out),
            in_specs=[vmem, vmem],
            out_specs=(pl.BlockSpec(memory_space=pltpu.HBM),) * 2,
            scratch_shapes=[dma((2,))],
            compiler_params=pltpu.CompilerParams(vmem_limit_bytes=4 * 1024 * 1024),
        )(*outs)
        return tuple(unflatten(o) for o in outs)

    return jax.shard_map(
        on_device,
        mesh=mesh,
        in_specs=(P("gz", None, "gy", "gx"), P("gz", None, "gy", "gx"), P("gz"), P(), P()),
        out_specs=(P("gz", None, "gy", "gx"), P("gz", None, "gy", "gx")),
        check_vma=False,
    )


VMEM_LIMIT = 40 * 1024 * 1024
```

```python
import functools

import jax
import jax.numpy as jnp
from jax import lax
from jax.experimental import pallas as pl
from jax.experimental.pallas import tpu as pltpu
from jax.sharding import PartitionSpec as P

SWEEPS = 3
REACH = 2 * SWEEPS + 1
POWERS = REACH + 1
SLOT = 8
MESH = pl.DeviceIdType.MESH


def total(terms):
    result = terms[0]
    for term in terms[1:]:
        result = result + term
    return result


def kernel(
    sizes, dims, material_hbm, sten_hbm, fac_hbm, load_hbm, start_hbm, out_u, out_r,
    material, sten, fac, load, start, coef, in_sem,
    mats, own_u, own_b, prev_u, prev_b, next_u, next_b, edge_out, edge_in, work_u, work_b, keep,
    sym_u, sym_b, sym_r, sym_y, sym_e, sym_c, maps, left, right, mine, outgoing, incoming, rim_out, rim_in, side_out, side_in,
    mat_ss, mat_rs, row_ss, row_rs, edge_ss, edge_rs, pass_ss, pass_rs, part_ss, part_rs, rim_ss, rim_rs, side_ss, side_rs,
):
    nz, ny, nx = sizes
    layers, comps, rows, lanes = dims
    planes = layers * comps
    deep = nz * layers
    width = lanes + 128
    gz, gy, gx = (lax.axis_index(name) for name in ("gz", "gy", "gx"))
    three = range(comps)
    half_group = -(-planes // 32) * 32
    depth = POWERS * half_group
    pending = []
    fetches = [
        pltpu.make_async_copy(src, dst, in_sem.at[i])
        for i, (src, dst) in enumerate((
            (start_hbm, start), (load_hbm, load), (sten_hbm, sten), (fac_hbm, fac), (material_hbm, material),
        ))
    ]
    for fetch in fetches:
        fetch.start()

    def at(z, y, x):
        return {"gz": z, "gy": y, "gx": x}

    def copy_if(cond, src, dst, ss, rs, target):
        copy = pltpu.make_async_remote_copy(
            src_ref=src, dst_ref=dst, send_sem=ss, recv_sem=rs,
            device_id=target, device_id_type=MESH,
        )

        if cond is True:
            copy.start()
        else:
            @pl.when(cond)
            def _():
                copy.start()

        pending.append((cond, copy))

    def arrive_if(cond, ref, ss, rs):
        copy = pltpu.make_async_remote_copy(
            src_ref=ref, dst_ref=ref, send_sem=ss, recv_sem=rs,
            device_id=at(gz, gy, gx), device_id_type=MESH,
        )
        if cond is True:
            copy.wait_recv()
        else:
            @pl.when(cond)
            def _():
                copy.wait_recv()

    has_prev_y, has_next_y = gy > 0, gy < ny - 1
    has_prev_x, has_next_x = gx > 0, gx < nx - 1
    sides_y = ((-1, has_prev_y), (1, has_next_y))
    sides_x = ((-1, has_prev_x), (1, has_next_x))

    barrier = pltpu.get_barrier_semaphore()
    peers = [(gz != j, at(j, gy, gx)) for j in range(nz)]
    peers += [(cond, at(gz, gy + step, gx)) for step, cond in sides_y]
    peers += [(cond, at(gz, gy, gx + step)) for step, cond in sides_x]
    for cond, target in peers:
        @pl.when(cond)
        def _(target=target):
            pl.semaphore_signal(barrier, inc=1, device_id=target, device_id_type=MESH)

    tiles = lanes // 128
    for own, given, fetch in ((own_u, start, fetches[0]), (own_b, load, fetches[1])):
        fetch.wait()
        for y in range(rows):
            for tile in range(tiles):
                own[y, :, tile * 128 : (tile + 1) * 128] = given[pl.ds(tile * rows + y, planes, stride=tiles * rows), :]

    def place(index):
        return (index * SLOT // 128) * 128, index * SLOT % 128

    tile_lane = lax.broadcasted_iota(jnp.int32, (planes, 128), 1)
    for side in range(2):
        for tile in range(edge_out.shape[2] // 128):
            packed = jnp.zeros((planes, 128), jnp.float32)
            for which, ref in enumerate((own_u, own_b)):
                for y in range(rows):
                    base, spot = place(which * rows + y)
                    if base != tile * 128:
                        continue
                    if side == 0:
                        piece = pltpu.roll(ref[y, :, 0:128], spot, 1) if spot else ref[y, :, 0:128]
                    else:
                        piece = pltpu.roll(ref[y, :, lanes - 128 : lanes], (spot + SLOT) % 128, 1)
                    inside = jnp.logical_and(tile_lane >= spot, tile_lane < spot + SLOT)
                    packed = jnp.where(inside, piece, packed)
            edge_out[side, :, tile * 128 : (tile + 1) * 128] = packed

    fetches[4].wait()
    pl.semaphore_wait(barrier, total([cond.astype(jnp.int32) for cond, _ in peers]))

    for j in range(nz):
        copy_if(gz != j, material, mats.at[gz], mat_ss.at[j], mat_rs.at[gz], at(j, gy, gx))
    strips = ((own_u, prev_u, next_u, REACH), (own_b, prev_b, next_b, REACH - 1))
    stages = rows // 2
    bounds = []
    for which, shared in ((0, 2), (1, 1)):
        reach = strips[which][3]
        enough = max(reach - stages + 1, 0)
        bounds.append(sorted({0, enough}) + list(range(enough + 1, reach + 1)))
    spans = [list(zip(b[:-1], b[1:])) for b in bounds]
    opening = [len([1 for _, last in spans[which] if last <= max(strips[which][3] - stages + 1, 0)]) for which in range(2)]

    def strip(which, step):
        own, prev, after, reach = strips[which]
        first, last = spans[which][step]
        return ((own.at[rows - last : rows - first], prev.at[reach - last : reach - first]),
                (own.at[first:last], after.at[first:last]))

    def send_rows(which, step):
        (out_up, in_up), (out_down, in_down) = strip(which, step)
        copy_if(has_next_y, out_up, in_up,
                row_ss.at[which, step, 0], row_rs.at[which, step, 0], at(gz, gy + 1, gx))
        copy_if(has_prev_y, out_down, in_down,
                row_ss.at[which, step, 1], row_rs.at[which, step, 1], at(gz, gy - 1, gx))

    early = [(0, step) for step in range(opening[0])]
    later = [(1, step) for step in range(opening[1])]
    for more in range(max(len(spans[0]) - opening[0], len(spans[1]) - opening[1])):
        later += [(w, opening[w] + more) for w in range(2) if opening[w] + more < len(spans[w])]
    for side, (step_x, cond_x) in enumerate(sides_x):
        copy_if(cond_x, edge_out.at[side], edge_in.at[1, 1 - side],
                edge_ss.at[1 - side], edge_rs.at[1 - side], at(gz, gy, gx + step_x))

    for which, step in early:
        send_rows(which, step)

    for layer in range(layers):
        mats[gz, layer] = material[layer]
    blocks = 3 * comps * comps
    for fetch in fetches[2:4]:
        fetch.wait()
    for first, table in ((0, sten), (blocks, fac)):
        for which in range(3):
            for i in three:
                for j in three:
                    for mat_id in range(coef.shape[0]):
                        spot = first + (which * comps + i) * comps + j
                        coef[mat_id, spot] = jnp.full((8, 128), table[which, i, j, mat_id], jnp.float32)
    for cond, refs in ((has_prev_y, (prev_u, prev_b)), (has_next_y, (next_u, next_b))):
        @pl.when(jnp.logical_not(cond))
        def _(refs=refs):
            for ref in refs:
                ref[...] = jnp.zeros_like(ref)
    for spot, (step_y, cond_y) in enumerate(sides_y):
        @pl.when(jnp.logical_not(cond_y))
        def _(spot=spot):
            edge_in[2 * spot] = jnp.zeros_like(edge_in[2 * spot])
    for side, (step_x, cond_x) in enumerate(sides_x):
        @pl.when(jnp.logical_not(cond_x))
        def _(side=side):
            edge_in[1, side] = jnp.zeros_like(edge_in[1, side])
    for side, (step_x, cond_x) in enumerate(sides_x):
        arrive_if(cond_x, edge_in.at[1, side], edge_ss.at[side], edge_rs.at[side])
    copy_if(has_next_y, edge_in.at[1], edge_in.at[0], pass_ss.at[0], pass_rs.at[0], at(gz, gy + 1, gx))
    copy_if(has_prev_y, edge_in.at[1], edge_in.at[2], pass_ss.at[1], pass_rs.at[1], at(gz, gy - 1, gx))
    for which, step in later:
        send_rows(which, step)
    wide_lane = lax.broadcasted_iota(jnp.int32, (planes, width), 1)
    inner = (wide_lane < lanes).astype(jnp.float32)
    inner = inner + jnp.where(
        jnp.logical_and(wide_lane >= lanes, wide_lane < lanes + SLOT), has_next_x.astype(jnp.float32), 0.0)
    inner = inner + jnp.where(wide_lane >= width - SLOT, has_prev_x.astype(jnp.float32), 0.0)
    keep[0] = inner * has_prev_y.astype(jnp.float32)
    keep[1] = inner
    keep[2] = inner * has_next_y.astype(jnp.float32)
    for part in range(3):
        for y in range(rows):
            right[part, y, 2 * depth - half_group :, :] = jnp.zeros((half_group, lanes), jnp.bfloat16)

    for j in range(nz):
        arrive_if(gz != j, mats.at[j], mat_ss.at[j], mat_rs.at[j])

    sub = lax.broadcasted_iota(jnp.int32, (8, 128), 0)
    lane = lax.broadcasted_iota(jnp.int32, (8, 128), 1)
    lowest = sub == 0

    def block(table, level, layer, which):
        z = layer * (2 if level else 1)
        mat_id = mats[z // layers, z % layers]
        first = which * comps * comps + (blocks if table is fac else 0)
        return [[coef[mat_id, first + i * comps + j] for j in three] for i in three]

    def times(mat, vec):
        return [total([mat[i][j] * vec[j] for j in three]) for i in three]

    def spread(x):
        return jnp.where(lowest, 0.0, pltpu.roll(x, 1, 0))

    for z in range(deep):
        here = gz == z // layers
        for c in three:
            plane = z % layers * comps + c
            spot = jnp.where(here, plane, -1 - half_group)
            sym_u[z * comps + c] = jnp.logical_and(lowest, lane == spot).astype(jnp.float32)
            sym_b[z * comps + c] = jnp.logical_and(lowest, lane == spot + half_group).astype(jnp.float32)

    def residual(level, field, source, count, layer):
        here = [field[layer * comps + c] for c in three]
        side = [spread(x) for x in here]
        vert = []
        for c in three:
            near = []
            if layer:
                near.append(field[(layer - 1) * comps + c])
            if layer < count - 1:
                near.append(field[(layer + 1) * comps + c])
            vert.append(0.25 * total(near) if level else total(near))
        a = times(block(sten, level, layer, 0), here)
        b = times(block(sten, level, layer, 1), side)
        d = times(block(sten, level, layer, 2), vert)
        return [source[layer * comps + c] - (a[c] - b[c] - d[c]) for c in three]

    def line_solve(level, resid, field, count, fresh):
        carry = None
        for layer in range(count):
            now = times(block(fac, level, layer, 0), resid(layer))
            if carry is not None:
                now = [a + b for a, b in zip(now, times(block(fac, level, layer, 1), carry))]
            for c in three:
                sym_y[layer * comps + c] = now[c]
            carry = now
        back = None
        for layer in reversed(range(count)):
            now = [sym_y[layer * comps + c] for c in three]
            if back is not None:
                now = [a + b for a, b in zip(now, times(block(fac, level, layer, 2), back))]
            for c in three:
                spot = layer * comps + c
                field[spot] = now[c] if fresh else field[spot] + now[c]
            back = now

    for sweep in range(SWEEPS):
        line_solve(0, lambda layer: residual(0, sym_u, sym_b, deep, layer), sym_u, deep, False)
    for k in range(deep // 2):
        pair = [residual(0, sym_u, sym_b, deep, 2 * k + step) for step in range(2)]
        for c in three:
            sym_c[k * comps + c] = pair[0][c] + pair[1][c]
    for sweep in range(SWEEPS):
        if sweep:
            source = functools.partial(residual, 1, sym_e, sym_c, deep // 2)
        else:
            def source(layer):
                return [sym_c[layer * comps + c] for c in three]
        line_solve(1, source, sym_e, deep // 2, sweep == 0)
    for z in range(deep):
        for c in three:
            sym_u[z * comps + c] = sym_u[z * comps + c] + sym_e[z // 2 * comps + c]
    for z in range(deep):
        value = residual(0, sym_u, sym_b, deep, z)
        first = z // layers * 2 * planes + z % layers * comps
        for c in three:
            maps[(first + c) * 8 : (first + c + 1) * 8, :] = sym_u[z * comps + c]
            spot = first + planes + c
            maps[spot * 8 : (spot + 1) * 8, :] = value[c]
    def thirds(x):
        high = x.astype(jnp.bfloat16)
        rest = x - high.astype(jnp.float32)
        middle = rest.astype(jnp.bfloat16)
        return high, middle, (rest - middle.astype(jnp.float32)).astype(jnp.bfloat16)

    size = 2 * planes
    count = nz * size
    map_lane = lax.broadcasted_iota(jnp.int32, (size, 128), 1)
    for i in range(nz):
        target = lax.rem(gz + 1 + i, nz)
        lines = [maps[pl.ds(target * size * 8 + power, size, stride=8), :] for power in range(POWERS)]
        for which in range(2):
            base = which * half_group
            inside = jnp.logical_and(map_lane >= base, map_lane < base + half_group)
            each = 128 // half_group
            for tile in range(POWERS // each):
                value = jnp.zeros((size, 128), jnp.float32)
                for part in range(each):
                    piece = jnp.where(inside, lines[tile * each + part], 0.0)
                    shift = (part * half_group - base) % 128
                    value = value + (pltpu.roll(piece, shift, 1) if shift else piece)
                first = which * depth + tile * 128
                for part, third in enumerate(thirds(value)):
                    left[part * count + i * size : part * count + (i + 1) * size, first : first + 128] = third

    def raw(which, y):
        own, prev, after, reach = strips[which]
        if y < 0:
            middle, step_y, line = prev[reach + y], -1, rows + y
        elif y < rows:
            middle, step_y, line = own[y], 0, y
        else:
            middle, step_y, line = after[y - rows], 1, y - rows
        base, spot = place(which * rows + line)
        west = pltpu.roll(edge_in[1 + step_y, 0, :, base : base + 128], (128 - SLOT - spot) % 128, 1)
        east = edge_in[1 + step_y, 1, :, base : base + 128]
        if spot:
            east = pltpu.roll(east, 128 - spot, 1)
        tail = jnp.where(tile_lane < SLOT, east, jnp.where(tile_lane >= 128 - SLOT, west, 0.0))
        return jnp.concatenate([middle, tail], axis=1)

    padding = jnp.zeros((half_group - planes, lanes), jnp.float32)
    done = set()

    def extend(which, known_rows):
        work, reach = (work_u, work_b)[which], strips[which][3]
        for power in range(reach + 1):
            for y in range(power - known_rows, rows + known_rows - power):
                if (which, power, y) in done:
                    continue
                done.add((which, power, y))
                if power == 0:
                    value = raw(which, y)
                else:
                    x = work[power - 1, y + reach]
                    value = pltpu.roll(x, 1, 1) + pltpu.roll(x, width - 1, 1)
                    value = value + (work[power - 1, y + reach - 1] + work[power - 1, y + reach + 1])
                    value = value * keep[0 if y < 0 else 1 if y < rows else 2]
                if power < reach:
                    work[power, y + reach] = value
                if 0 <= y < rows:
                    first = which * depth + power * half_group
                    cell = value[:, :lanes]
                    if half_group > planes:
                        cell = jnp.concatenate([cell, padding], axis=0)
                    for part, third in enumerate(thirds(cell)):
                        right[part, y, first : first + half_group, :] = third

    def take(which, step):
        (_, in_up), (_, in_down) = strip(which, step)
        arrive_if(has_prev_y, in_up, row_ss.at[which, step, 0], row_rs.at[which, step, 0])
        arrive_if(has_next_y, in_down, row_ss.at[which, step, 1], row_rs.at[which, step, 1])
        extend(which, spans[which][step][1])

    for which in range(2):
        extend(which, 0)
    for spot, (step_y, cond_y) in enumerate(sides_y):
        arrive_if(cond_y, edge_in.at[2 * spot], pass_ss.at[spot], pass_rs.at[spot])
    rim_id = lax.broadcasted_iota(jnp.int32, (8, lanes), 0)
    rim_low, rim_high = rim_id < comps, rim_id >= 8 - comps
    columns = [jnp.zeros((planes, 128), jnp.float32)] * (nz - 1)

    def side_tile(field, y):
        first = jnp.where(tile_lane == 2 * y, pltpu.roll(field[:, :128], 2 * y, 1), 0.0)
        last = jnp.where(tile_lane == 2 * y + 1, pltpu.roll(field[:, lanes - 128 :], (2 * y + 2) % 128, 1), 0.0)
        return first + last

    for stage in range(stages):
        for which in range(2):
            first = opening[which] + stage - 1 if stage else 0
            for step in range(first, opening[which] + stage):
                if step < len(spans[which]):
                    take(which, step)
        for y in (stages - 1 - stage, stages + stage):
            pieces = []
            for part in (2, 1, 0):
                product = jnp.dot(left[: (3 - part) * count], right[part, y], preferred_element_type=jnp.float32)
                pieces += [product[k * count : (k + 1) * count] for k in reversed(range(3 - part))]
            value = total(pieces)
            for i in range(nz - 1):
                target = at(lax.rem(gz + 1 + i, nz), gy, gx)
                share = value[i * size : (i + 1) * size]
                whole = y in (0, rows - 1)
                outgoing[i, y] = share
                amount = size if whole else planes
                copy_if(True, outgoing.at[i, y, 0:amount], incoming.at[i, y, 0:amount],
                        part_ss.at[i, y], part_rs.at[i, y], target)
                if whole:
                    continue
                low, high = share[planes : planes + 8], share[size - 8 : size]
                upper = y >= stages
                if nz == 2:
                    ends = jnp.where(gz == 1, pltpu.roll(high, comps, 0), low)
                    if upper:
                        ends = jnp.where(rim_id < 4, held, pltpu.roll(ends, 4, 0))
                    held = ends
                else:
                    ends = jnp.where(rim_low, low, high)
                if nz > 2 or upper:
                    spot = (i, stage, int(upper) if nz > 2 else 0)
                    rim_out[spot] = ends
                    copy_if(True, rim_out.at[spot], rim_in.at[spot], rim_ss.at[spot], rim_rs.at[spot], target)
                columns[i] = columns[i] + side_tile(share[planes:], y)
                if stage == stages - 2 and y == stages + stage:
                    side_out[i] = columns[i]
                    copy_if(True, side_out.at[i], side_in.at[i], side_ss.at[i], side_rs.at[i], target)
            mine[y] = value[(nz - 1) * size :]
    rest_id = lax.broadcasted_iota(jnp.int32, (planes, 128), 0)
    taken = set()
    open_low, open_high = (gz == 0, gz == 1) if nz == 2 else (False, False)
    for y in [y for stage in range(stages) for y in (stages - 1 - stage, stages + stage)]:
        value = mine[y]
        whole = y in (0, rows - 1)
        solved, rest = value[:planes], value[planes:]
        for i in range(nz - 1):
            amount = size if whole else planes
            arrive_if(True, incoming.at[i, y, 0:amount], part_ss.at[i, y], part_rs.at[i, y])
            solved = solved + incoming[i, y, 0:planes]
            if whole:
                rest = rest + incoming[i, y, planes:size]
        for tile in range(tiles):
            spots = pl.ds(tile * rows + y, planes, stride=tiles * rows)
            out_u[spots, :] = solved[:, tile * 128 : (tile + 1) * 128]
            if whole:
                out_r[spots, :] = rest[:, tile * 128 : (tile + 1) * 128]
        if y == 1:
            for i in range(nz - 1):
                arrive_if(True, side_in.at[i], side_ss.at[i], side_rs.at[i])
        if y == rows - 2:
            sides = total([side_in[i] for i in range(nz - 1)]) if nz > 1 else jnp.zeros((planes, 128), jnp.float32)
            for line in range(1, rows - 1):
                rest = mine[line][planes:]
                ends = [jnp.zeros((8, lanes), jnp.float32)] * 2
                upper = line >= stages
                stage = line - stages if upper else stages - 1 - line
                for i in range(nz - 1):
                    spot = (i, stage, int(upper) if nz > 2 else 0)
                    if spot not in taken:
                        taken.add(spot)
                        arrive_if(True, rim_in.at[spot], rim_ss.at[spot], rim_rs.at[spot])
                    given = rim_in[spot]
                    if nz == 2:
                        given = pltpu.roll(given, 4, 0) if upper else given
                        ends = [jnp.where(jnp.logical_and(rim_low, gz == 1), given, 0.0),
                                jnp.where(jnp.logical_and(rim_high, gz == 0), pltpu.roll(given, 8 - comps, 0), 0.0)]
                    else:
                        ends = [ends[0] + jnp.where(rim_low, given, 0.0), ends[1] + jnp.where(rim_high, given, 0.0)]
                cut = [rest[:8] + ends[0], rest[8 : planes - 8], rest[planes - 8 :] + ends[1]]
                rest = jnp.concatenate(cut, axis=0)
                inner_side = jnp.logical_and(
                    jnp.logical_or(rest_id >= comps, open_low), jnp.logical_or(rest_id < planes - comps, open_high))
                for tile in range(tiles):
                    part = rest[:, tile * 128 : (tile + 1) * 128]
                    if tile == 0:
                        add = pltpu.roll(sides, 128 - 2 * line, 1)
                        part = part + jnp.where(jnp.logical_and(inner_side, tile_lane == 0), add, 0.0)
                    if tile == tiles - 1:
                        add = pltpu.roll(sides, 126 - 2 * line, 1)
                        part = part + jnp.where(jnp.logical_and(inner_side, tile_lane == 127), add, 0.0)
                    out_r[pl.ds(tile * rows + line, planes, stride=tiles * rows), :] = part

    row_id = lax.broadcasted_iota(jnp.int32, (rows, 128), 0)
    lane_id = lax.broadcasted_iota(jnp.int32, (rows, 128), 1)
    row_rim = jnp.logical_or(row_id == 0, row_id == rows - 1)

    def solution_tile(layer, c, tile):
        first = ((layer * comps + c) * tiles + tile) * rows
        return pl.ds(first, rows)

    def shares(layer, first):
        mat_id = mats[gz, layer]
        return [[coef[mat_id, first + i * comps + j] for j in three] for i in three]

    for layer in range(layers) if nz == 2 else range(1, layers - 1):
        mat = [shares(layer, which * comps * comps) for which in range(3)]
        for tile in range(tiles):
            here, side, vert = [], [], []
            for c in three:
                x = out_u[solution_tile(layer, c, tile), :]
                west = out_u[solution_tile(layer, c, tile - 1), :] if tile else x
                east = out_u[solution_tile(layer, c, tile + 1), :] if tile < tiles - 1 else x
                beside = jnp.where(lane_id == 127, west, x), jnp.where(lane_id == 0, east, x)
                around = pltpu.roll(beside[0], 1, 1) + pltpu.roll(beside[1], 127, 1)
                here.append(x)
                side.append(around + (pltpu.roll(x, 1, 0) + pltpu.roll(x, rows - 1, 0)))
                near = [out_u[solution_tile(z, c, tile), :] for z in (layer - 1, layer + 1) if 0 <= z < layers]
                vert.append(total(near))
            a, b, d = (times(mat[which], vec) for which, vec in enumerate((here, side, vert)))
            rim = row_rim
            if layer in (0, layers - 1):
                rim = jnp.logical_or(rim, jnp.logical_not(open_high if layer else open_low))
            if tile == 0:
                rim = jnp.logical_or(rim, lane_id == 0)
            if tile == tiles - 1:
                rim = jnp.logical_or(rim, lane_id == 127)
            for c in three:
                spot = solution_tile(layer, c, tile)
                first = ((layer * comps + c) * tiles + tile) * rows
                value = load[first : first + rows, :] - (a[c] - b[c] - d[c])
                out_r[spot, :] = jnp.where(rim, out_r[spot, :], value)
    for cond, copy in pending:
        if cond is True:
            copy.wait_send()
        else:
            @pl.when(cond)
            def _(copy=copy):
                copy.wait_send()


def put(from_u, from_r, to_u, to_r, sem):
    copies = [pltpu.make_async_copy(src, dst, sem.at[i]) for i, (src, dst) in enumerate(((from_u, to_u), (from_r, to_r)))]
    for copy in copies:
        copy.start()
    for copy in copies:
        copy.wait()


def solution(mesh):
    sizes = tuple(mesh.shape[name] for name in ("gz", "gy", "gx"))
    nz = sizes[0]

    def on_device(right_side, start_field, layer_material, stiffness, line_factors):
        dims = right_side.shape
        layers, comps, rows, lanes = dims
        planes = layers * comps
        deep = nz * layers
        half_group = -(-planes // 32) * 32
        depth = POWERS * 2 * half_group
        packed = -(-2 * rows * SLOT // 128) * 128
        f32 = jnp.float32
        vmem = pl.BlockSpec(memory_space=pltpu.VMEM)
        dma = pltpu.SemaphoreType.DMA
        others = max(nz - 1, 1)
        symbol = pltpu.VMEM((deep * comps, 8, 128), f32)
        tables = (3, comps, comps, stiffness.shape[0])
        flat = (planes * rows * lanes // 128, 128)
        scratch = [pltpu.SMEM((layers,), jnp.int32)]
        scratch += [pltpu.SMEM(tables, f32)] * 2
        scratch += [pltpu.VMEM(flat, f32)] * 2
        scratch += [pltpu.VMEM((tables[3], 2 * 3 * comps * comps, 8, 128), f32), dma((5,))]
        scratch += [pltpu.SMEM((nz, layers), jnp.int32)]
        scratch += [pltpu.VMEM((rows, planes, lanes), f32)] * 2
        scratch += [pltpu.VMEM((n, planes, lanes), f32) for n in (REACH, REACH - 1, REACH, REACH - 1)]
        scratch += [
            pltpu.VMEM((2, planes, packed), f32),
            pltpu.VMEM((3, 2, planes, packed), f32),
            pltpu.VMEM((REACH, rows + 2 * REACH, planes, lanes + 128), f32),
            pltpu.VMEM((REACH - 1, rows + 2 * REACH - 2, planes, lanes + 128), f32),
            pltpu.VMEM((3, planes, lanes + 128), f32),
        ]
        scratch += [symbol] * 6
        scratch += [
            pltpu.VMEM((nz * 2 * planes * 8, 128), f32),
            pltpu.VMEM((3 * nz * 2 * planes, depth), jnp.bfloat16),
            pltpu.VMEM((3, rows, depth, lanes), jnp.bfloat16),
            pltpu.VMEM((rows, 2 * planes, lanes), f32),
            pltpu.VMEM((others, rows, 2 * planes, lanes), f32),
            pltpu.VMEM((others, rows, 2 * planes, lanes), f32),
        ]
        scratch += [pltpu.VMEM((others, rows // 2, 2, 8, lanes), f32)] * 2 + [pltpu.VMEM((others, planes, 128), f32)] * 2
        scratch += [dma((nz,))] * 2 + [dma((2, REACH, 2))] * 2 + [dma((2,))] * 4 + [dma((others, rows))] * 2 + [dma((others, rows // 2, 2))] * 2 + [dma((others,))] * 2
        tiled = (layers, comps, rows, lanes // 128, 128)

        def flatten(x):
            return x.reshape(tiled).transpose(0, 1, 3, 2, 4).reshape(-1, 128)

        def unflatten(x):
            split = x.reshape(layers, comps, lanes // 128, rows, 128)
            return split.transpose(0, 1, 3, 2, 4).reshape(dims)

        out = jax.ShapeDtypeStruct(flat, f32)
        given = (layer_material, stiffness.transpose(1, 2, 3, 0), line_factors.transpose(1, 2, 3, 0),
                 flatten(right_side), flatten(start_field))
        given = [pltpu.with_memory_space_constraint(x, pltpu.HBM) for x in given]
        outs = pl.pallas_call(
            functools.partial(kernel, sizes, dims),
            out_shape=(out, out),
            in_specs=[pl.BlockSpec(memory_space=pltpu.HBM)] * 5,
            out_specs=(vmem, vmem),
            scratch_shapes=scratch,
            compiler_params=pltpu.CompilerParams(
                collective_id=0, has_side_effects=True, vmem_limit_bytes=VMEM_LIMIT),
        )(*given)
        outs = pl.pallas_call(
            put,
            out_shape=(out, out),
            in_specs=[vmem, vmem],
            out_specs=(pl.BlockSpec(memory_space=pltpu.HBM),) * 2,
            scratch_shapes=[dma((2,))],
            compiler_params=pltpu.CompilerParams(vmem_limit_bytes=4 * 1024 * 1024),
        )(*outs)
        return tuple(unflatten(o) for o in outs)

    return jax.shard_map(
        on_device,
        mesh=mesh,
        in_specs=(P("gz", None, "gy", "gx"), P("gz", None, "gy", "gx"), P("gz"), P(), P()),
        out_specs=(P("gz", None, "gy", "gx"), P("gz", None, "gy", "gx")),
        check_vma=False,
    )


VMEM_LIMIT = 40 * 1024 * 1024
```

```python
import functools

import jax
import jax.numpy as jnp
from jax import lax
from jax.experimental import pallas as pl
from jax.experimental.pallas import tpu as pltpu
from jax.sharding import PartitionSpec as P

SWEEPS = 3
REACH = 2 * SWEEPS + 1
POWERS = REACH + 1
SLOT = 8
MESH = pl.DeviceIdType.MESH


def total(terms):
    result = terms[0]
    for term in terms[1:]:
        result = result + term
    return result


def kernel(
    sizes, dims, material_hbm, sten_hbm, fac_hbm, load_hbm, start_hbm, out_u, out_r,
    material, sten, fac, load, start, coef, in_sem,
    mats, own_u, own_b, prev_u, prev_b, next_u, next_b, edge_out, edge_in, work_u, work_b, keep,
    sym_u, sym_b, sym_r, sym_y, sym_e, sym_c, maps, left, right, mine, outgoing, incoming, rim_out, rim_in, side_out, side_in,
    mat_ss, mat_rs, row_ss, row_rs, edge_ss, edge_rs, pass_ss, pass_rs, part_ss, part_rs, rim_ss, rim_rs, side_ss, side_rs,
):
    nz, ny, nx = sizes
    layers, comps, rows, lanes = dims
    planes = layers * comps
    deep = nz * layers
    width = lanes + 128
    gz, gy, gx = (lax.axis_index(name) for name in ("gz", "gy", "gx"))
    three = range(comps)
    half_group = -(-planes // 32) * 32
    depth = POWERS * half_group
    pending = []
    fetches = [
        pltpu.make_async_copy(src, dst, in_sem.at[i])
        for i, (src, dst) in enumerate((
            (start_hbm, start), (load_hbm, load), (sten_hbm, sten), (fac_hbm, fac), (material_hbm, material),
        ))
    ]
    for fetch in fetches:
        fetch.start()

    def at(z, y, x):
        return {"gz": z, "gy": y, "gx": x}

    def copy_if(cond, src, dst, ss, rs, target):
        copy = pltpu.make_async_remote_copy(
            src_ref=src, dst_ref=dst, send_sem=ss, recv_sem=rs,
            device_id=target, device_id_type=MESH,
        )

        if cond is True:
            copy.start()
        else:
            @pl.when(cond)
            def _():
                copy.start()

        pending.append((cond, copy))

    def arrive_if(cond, ref, ss, rs):
        copy = pltpu.make_async_remote_copy(
            src_ref=ref, dst_ref=ref, send_sem=ss, recv_sem=rs,
            device_id=at(gz, gy, gx), device_id_type=MESH,
        )
        if cond is True:
            copy.wait_recv()
        else:
            @pl.when(cond)
            def _():
                copy.wait_recv()

    has_prev_y, has_next_y = gy > 0, gy < ny - 1
    has_prev_x, has_next_x = gx > 0, gx < nx - 1
    sides_y = ((-1, has_prev_y), (1, has_next_y))
    sides_x = ((-1, has_prev_x), (1, has_next_x))

    barrier = pltpu.get_barrier_semaphore()
    peers = [(gz != j, at(j, gy, gx)) for j in range(nz)]
    peers += [(cond, at(gz, gy + step, gx)) for step, cond in sides_y]
    peers += [(cond, at(gz, gy, gx + step)) for step, cond in sides_x]
    for cond, target in peers:
        @pl.when(cond)
        def _(target=target):
            pl.semaphore_signal(barrier, inc=1, device_id=target, device_id_type=MESH)

    tiles = lanes // 128
    for own, given, fetch in ((own_u, start, fetches[0]), (own_b, load, fetches[1])):
        fetch.wait()
        for y in range(rows):
            for tile in range(tiles):
                own[y, :, tile * 128 : (tile + 1) * 128] = given[pl.ds(tile * rows + y, planes, stride=tiles * rows), :]

    def place(index):
        return (index * SLOT // 128) * 128, index * SLOT % 128

    tile_lane = lax.broadcasted_iota(jnp.int32, (planes, 128), 1)
    for side in range(2):
        for tile in range(edge_out.shape[2] // 128):
            packed = jnp.zeros((planes, 128), jnp.float32)
            for which, ref in enumerate((own_u, own_b)):
                for y in range(rows):
                    base, spot = place(which * rows + y)
                    if base != tile * 128:
                        continue
                    if side == 0:
                        piece = pltpu.roll(ref[y, :, 0:128], spot, 1) if spot else ref[y, :, 0:128]
                    else:
                        piece = pltpu.roll(ref[y, :, lanes - 128 : lanes], (spot + SLOT) % 128, 1)
                    inside = jnp.logical_and(tile_lane >= spot, tile_lane < spot + SLOT)
                    packed = jnp.where(inside, piece, packed)
            edge_out[side, :, tile * 128 : (tile + 1) * 128] = packed

    fetches[4].wait()
    pl.semaphore_wait(barrier, total([cond.astype(jnp.int32) for cond, _ in peers]))

    for j in range(nz):
        copy_if(gz != j, material, mats.at[gz], mat_ss.at[j], mat_rs.at[gz], at(j, gy, gx))
    strips = ((own_u, prev_u, next_u, REACH), (own_b, prev_b, next_b, REACH - 1))
    stages = rows // 2
    bounds = []
    for which, shared in ((0, 2), (1, 1)):
        reach = strips[which][3]
        enough = max(reach - stages + 1, 0)
        bounds.append(sorted({0, enough}) + list(range(enough + 1, reach + 1)))
    spans = [list(zip(b[:-1], b[1:])) for b in bounds]
    opening = [len([1 for _, last in spans[which] if last <= max(strips[which][3] - stages + 1, 0)]) for which in range(2)]

    def strip(which, step):
        own, prev, after, reach = strips[which]
        first, last = spans[which][step]
        return ((own.at[rows - last : rows - first], prev.at[reach - last : reach - first]),
                (own.at[first:last], after.at[first:last]))

    def send_rows(which, step):
        (out_up, in_up), (out_down, in_down) = strip(which, step)
        copy_if(has_next_y, out_up, in_up,
                row_ss.at[which, step, 0], row_rs.at[which, step, 0], at(gz, gy + 1, gx))
        copy_if(has_prev_y, out_down, in_down,
                row_ss.at[which, step, 1], row_rs.at[which, step, 1], at(gz, gy - 1, gx))

    early = [(0, step) for step in range(opening[0])]
    later = [(1, step) for step in range(opening[1])]
    for more in range(max(len(spans[0]) - opening[0], len(spans[1]) - opening[1])):
        later += [(w, opening[w] + more) for w in range(2) if opening[w] + more < len(spans[w])]
    for side, (step_x, cond_x) in enumerate(sides_x):
        copy_if(cond_x, edge_out.at[side], edge_in.at[1, 1 - side],
                edge_ss.at[1 - side], edge_rs.at[1 - side], at(gz, gy, gx + step_x))

    for which, step in early:
        send_rows(which, step)

    for layer in range(layers):
        mats[gz, layer] = material[layer]
    blocks = 3 * comps * comps
    for fetch in fetches[2:4]:
        fetch.wait()
    for first, table in ((0, sten), (blocks, fac)):
        for which in range(3):
            for i in three:
                for j in three:
                    for mat_id in range(coef.shape[0]):
                        spot = first + (which * comps + i) * comps + j
                        coef[mat_id, spot] = jnp.full((8, 128), table[which, i, j, mat_id], jnp.float32)
    for cond, refs in ((has_prev_y, (prev_u, prev_b)), (has_next_y, (next_u, next_b))):
        @pl.when(jnp.logical_not(cond))
        def _(refs=refs):
            for ref in refs:
                ref[...] = jnp.zeros_like(ref)
    for spot, (step_y, cond_y) in enumerate(sides_y):
        @pl.when(jnp.logical_not(cond_y))
        def _(spot=spot):
            edge_in[2 * spot] = jnp.zeros_like(edge_in[2 * spot])
    for side, (step_x, cond_x) in enumerate(sides_x):
        @pl.when(jnp.logical_not(cond_x))
        def _(side=side):
            edge_in[1, side] = jnp.zeros_like(edge_in[1, side])
    for side, (step_x, cond_x) in enumerate(sides_x):
        arrive_if(cond_x, edge_in.at[1, side], edge_ss.at[side], edge_rs.at[side])
    copy_if(has_next_y, edge_in.at[1], edge_in.at[0], pass_ss.at[0], pass_rs.at[0], at(gz, gy + 1, gx))
    copy_if(has_prev_y, edge_in.at[1], edge_in.at[2], pass_ss.at[1], pass_rs.at[1], at(gz, gy - 1, gx))
    for which, step in later:
        send_rows(which, step)
    wide_lane = lax.broadcasted_iota(jnp.int32, (planes, width), 1)
    inner = (wide_lane < lanes).astype(jnp.float32)
    inner = inner + jnp.where(
        jnp.logical_and(wide_lane >= lanes, wide_lane < lanes + SLOT), has_next_x.astype(jnp.float32), 0.0)
    inner = inner + jnp.where(wide_lane >= width - SLOT, has_prev_x.astype(jnp.float32), 0.0)
    keep[0] = inner * has_prev_y.astype(jnp.float32)
    keep[1] = inner
    keep[2] = inner * has_next_y.astype(jnp.float32)
    for part in range(3):
        for y in range(rows):
            right[part, y, 2 * depth - half_group :, :] = jnp.zeros((half_group, lanes), jnp.bfloat16)

    for j in range(nz):
        arrive_if(gz != j, mats.at[j], mat_ss.at[j], mat_rs.at[j])

    sub = lax.broadcasted_iota(jnp.int32, (8, 128), 0)
    lane = lax.broadcasted_iota(jnp.int32, (8, 128), 1)
    lowest = sub == 0

    def block(table, level, layer, which):
        z = layer * (2 if level else 1)
        mat_id = mats[z // layers, z % layers]
        first = which * comps * comps + (blocks if table is fac else 0)
        return [[coef[mat_id, first + i * comps + j] for j in three] for i in three]

    def times(mat, vec):
        return [total([mat[i][j] * vec[j] for j in three]) for i in three]

    def spread(x):
        return jnp.where(lowest, 0.0, pltpu.roll(x, 1, 0))

    for z in range(deep):
        here = gz == z // layers
        for c in three:
            plane = z % layers * comps + c
            spot = jnp.where(here, plane, -1 - half_group)
            sym_u[z * comps + c] = jnp.logical_and(lowest, lane == spot).astype(jnp.float32)
            sym_b[z * comps + c] = jnp.logical_and(lowest, lane == spot + half_group).astype(jnp.float32)

    def residual(level, field, source, count, layer):
        here = [field[layer * comps + c] for c in three]
        side = [spread(x) for x in here]
        vert = []
        for c in three:
            near = []
            if layer:
                near.append(field[(layer - 1) * comps + c])
            if layer < count - 1:
                near.append(field[(layer + 1) * comps + c])
            vert.append(0.25 * total(near) if level else total(near))
        a = times(block(sten, level, layer, 0), here)
        b = times(block(sten, level, layer, 1), side)
        d = times(block(sten, level, layer, 2), vert)
        return [source[layer * comps + c] - (a[c] - b[c] - d[c]) for c in three]

    def line_solve(level, resid, field, count, fresh):
        carry = None
        for layer in range(count):
            now = times(block(fac, level, layer, 0), resid(layer))
            if carry is not None:
                now = [a + b for a, b in zip(now, times(block(fac, level, layer, 1), carry))]
            for c in three:
                sym_y[layer * comps + c] = now[c]
            carry = now
        back = None
        for layer in reversed(range(count)):
            now = [sym_y[layer * comps + c] for c in three]
            if back is not None:
                now = [a + b for a, b in zip(now, times(block(fac, level, layer, 2), back))]
            for c in three:
                spot = layer * comps + c
                field[spot] = now[c] if fresh else field[spot] + now[c]
            back = now

    for sweep in range(SWEEPS):
        line_solve(0, lambda layer: residual(0, sym_u, sym_b, deep, layer), sym_u, deep, False)
    for k in range(deep // 2):
        pair = [residual(0, sym_u, sym_b, deep, 2 * k + step) for step in range(2)]
        for c in three:
            sym_c[k * comps + c] = pair[0][c] + pair[1][c]
    for sweep in range(SWEEPS):
        if sweep:
            source = functools.partial(residual, 1, sym_e, sym_c, deep // 2)
        else:
            def source(layer):
                return [sym_c[layer * comps + c] for c in three]
        line_solve(1, source, sym_e, deep // 2, sweep == 0)
    for z in range(deep):
        for c in three:
            sym_u[z * comps + c] = sym_u[z * comps + c] + sym_e[z // 2 * comps + c]
    for z in range(deep):
        value = residual(0, sym_u, sym_b, deep, z)
        first = z // layers * 2 * planes + z % layers * comps
        for c in three:
            maps[(first + c) * 8 : (first + c + 1) * 8, :] = sym_u[z * comps + c]
            spot = first + planes + c
            maps[spot * 8 : (spot + 1) * 8, :] = value[c]
    def thirds(x):
        high = x.astype(jnp.bfloat16)
        rest = x - high.astype(jnp.float32)
        middle = rest.astype(jnp.bfloat16)
        return high, middle, (rest - middle.astype(jnp.float32)).astype(jnp.bfloat16)

    size = 2 * planes
    count = nz * size
    map_lane = lax.broadcasted_iota(jnp.int32, (size, 128), 1)
    for i in range(nz):
        target = lax.rem(gz + 1 + i, nz)
        lines = [maps[pl.ds(target * size * 8 + power, size, stride=8), :] for power in range(POWERS)]
        for which in range(2):
            base = which * half_group
            inside = jnp.logical_and(map_lane >= base, map_lane < base + half_group)
            each = 128 // half_group
            for tile in range(POWERS // each):
                value = jnp.zeros((size, 128), jnp.float32)
                for part in range(each):
                    piece = jnp.where(inside, lines[tile * each + part], 0.0)
                    shift = (part * half_group - base) % 128
                    value = value + (pltpu.roll(piece, shift, 1) if shift else piece)
                first = which * depth + tile * 128
                for part, third in enumerate(thirds(value)):
                    left[part * count + i * size : part * count + (i + 1) * size, first : first + 128] = third

    def raw(which, y):
        own, prev, after, reach = strips[which]
        if y < 0:
            middle, step_y, line = prev[reach + y], -1, rows + y
        elif y < rows:
            middle, step_y, line = own[y], 0, y
        else:
            middle, step_y, line = after[y - rows], 1, y - rows
        base, spot = place(which * rows + line)
        west = pltpu.roll(edge_in[1 + step_y, 0, :, base : base + 128], (128 - SLOT - spot) % 128, 1)
        east = edge_in[1 + step_y, 1, :, base : base + 128]
        if spot:
            east = pltpu.roll(east, 128 - spot, 1)
        tail = jnp.where(tile_lane < SLOT, east, jnp.where(tile_lane >= 128 - SLOT, west, 0.0))
        return jnp.concatenate([middle, tail], axis=1)

    padding = jnp.zeros((half_group - planes, lanes), jnp.float32)
    done = set()

    def put_powers(which, power, y, cell):
        first = which * depth + power * half_group
        if half_group > planes:
            cell = jnp.concatenate([cell, padding], axis=0)
        for part, third in enumerate(thirds(cell)):
            right[part, y, first : first + half_group, :] = third

    def extend(which, known_rows):
        work, reach = (work_u, work_b)[which], strips[which][3]
        for power in range(reach + 1):
            for y in range(power - known_rows, rows + known_rows - power):
                if (which, power, y) in done:
                    continue
                done.add((which, power, y))
                if power == 0:
                    value = raw(which, y)
                else:
                    x = work[power - 1, y + reach]
                    if power == reach:
                        parts = [x[:, k : k + 128] for k in range(0, width, 128)]
                        west = [jnp.where(tile_lane == 127, parts[k - 1], parts[k]) for k in range(tiles)]
                        east = [jnp.where(tile_lane == 0, parts[k + 1], parts[k]) for k in range(tiles)]
                        near = [pltpu.roll(a, 1, 1) + pltpu.roll(b, 127, 1) for a, b in zip(west, east)]
                        cross = work[power - 1, y + reach - 1, :, :lanes] + work[power - 1, y + reach + 1, :, :lanes]
                        value = jnp.concatenate(near, axis=1) + cross
                        put_powers(which, power, y, value)
                        continue
                    value = pltpu.roll(x, 1, 1) + pltpu.roll(x, width - 1, 1)
                    value = value + (work[power - 1, y + reach - 1] + work[power - 1, y + reach + 1])
                    value = value * keep[0 if y < 0 else 1 if y < rows else 2]
                if power < reach:
                    work[power, y + reach] = value
                if 0 <= y < rows:
                    put_powers(which, power, y, value[:, :lanes])

    def take(which, step):
        (_, in_up), (_, in_down) = strip(which, step)
        arrive_if(has_prev_y, in_up, row_ss.at[which, step, 0], row_rs.at[which, step, 0])
        arrive_if(has_next_y, in_down, row_ss.at[which, step, 1], row_rs.at[which, step, 1])
        extend(which, spans[which][step][1])

    for which in range(2):
        extend(which, 0)
    for spot, (step_y, cond_y) in enumerate(sides_y):
        arrive_if(cond_y, edge_in.at[2 * spot], pass_ss.at[spot], pass_rs.at[spot])
    rim_id = lax.broadcasted_iota(jnp.int32, (8, lanes), 0)
    rim_low, rim_high = rim_id < comps, rim_id >= 8 - comps
    columns = [jnp.zeros((planes, 128), jnp.float32)] * (nz - 1)

    def side_tile(field, y):
        first = jnp.where(tile_lane == 2 * y, pltpu.roll(field[:, :128], 2 * y, 1), 0.0)
        last = jnp.where(tile_lane == 2 * y + 1, pltpu.roll(field[:, lanes - 128 :], (2 * y + 2) % 128, 1), 0.0)
        return first + last

    for stage in range(stages):
        for which in range(2):
            first = opening[which] + stage - 1 if stage else 0
            for step in range(first, opening[which] + stage):
                if step < len(spans[which]):
                    take(which, step)
        for y in (stages - 1 - stage, stages + stage):
            pieces = []
            for part in (2, 1, 0):
                product = jnp.dot(left[: (3 - part) * count], right[part, y], preferred_element_type=jnp.float32)
                pieces += [product[k * count : (k + 1) * count] for k in reversed(range(3 - part))]
            value = total(pieces)
            for i in range(nz - 1):
                target = at(lax.rem(gz + 1 + i, nz), gy, gx)
                share = value[i * size : (i + 1) * size]
                whole = y in (0, rows - 1)
                outgoing[i, y] = share
                amount = size if whole else planes
                copy_if(True, outgoing.at[i, y, 0:amount], incoming.at[i, y, 0:amount],
                        part_ss.at[i, y], part_rs.at[i, y], target)
                if whole:
                    continue
                low, high = share[planes : planes + 8], share[size - 8 : size]
                upper = y >= stages
                if nz == 2:
                    ends = jnp.where(gz == 1, pltpu.roll(high, comps, 0), low)
                    if upper:
                        ends = jnp.where(rim_id < 4, held, pltpu.roll(ends, 4, 0))
                    held = ends
                else:
                    ends = jnp.where(rim_low, low, high)
                if nz > 2 or upper:
                    spot = (i, stage, int(upper) if nz > 2 else 0)
                    rim_out[spot] = ends
                    copy_if(True, rim_out.at[spot], rim_in.at[spot], rim_ss.at[spot], rim_rs.at[spot], target)
                columns[i] = columns[i] + side_tile(share[planes:], y)
                if stage == stages - 2 and y == stages + stage:
                    side_out[i] = columns[i]
                    copy_if(True, side_out.at[i], side_in.at[i], side_ss.at[i], side_rs.at[i], target)
            mine[y] = value[(nz - 1) * size :]
    rest_id = lax.broadcasted_iota(jnp.int32, (planes, 128), 0)
    taken = set()
    open_low, open_high = (gz == 0, gz == 1) if nz == 2 else (False, False)
    for y in [y for stage in range(stages) for y in (stages - 1 - stage, stages + stage)]:
        value = mine[y]
        whole = y in (0, rows - 1)
        solved, rest = value[:planes], value[planes:]
        for i in range(nz - 1):
            amount = size if whole else planes
            arrive_if(True, incoming.at[i, y, 0:amount], part_ss.at[i, y], part_rs.at[i, y])
            solved = solved + incoming[i, y, 0:planes]
            if whole:
                rest = rest + incoming[i, y, planes:size]
        for tile in range(tiles):
            spots = pl.ds(tile * rows + y, planes, stride=tiles * rows)
            out_u[spots, :] = solved[:, tile * 128 : (tile + 1) * 128]
            if whole:
                out_r[spots, :] = rest[:, tile * 128 : (tile + 1) * 128]
        if y == 1:
            for i in range(nz - 1):
                arrive_if(True, side_in.at[i], side_ss.at[i], side_rs.at[i])
        if y == rows - 2:
            sides = total([side_in[i] for i in range(nz - 1)]) if nz > 1 else jnp.zeros((planes, 128), jnp.float32)
            for line in range(1, rows - 1):
                rest = mine[line][planes:]
                ends = [jnp.zeros((8, lanes), jnp.float32)] * 2
                upper = line >= stages
                stage = line - stages if upper else stages - 1 - line
                for i in range(nz - 1):
                    spot = (i, stage, int(upper) if nz > 2 else 0)
                    if spot not in taken:
                        taken.add(spot)
                        arrive_if(True, rim_in.at[spot], rim_ss.at[spot], rim_rs.at[spot])
                    given = rim_in[spot]
                    if nz == 2:
                        given = pltpu.roll(given, 4, 0) if upper else given
                        ends = [jnp.where(jnp.logical_and(rim_low, gz == 1), given, 0.0),
                                jnp.where(jnp.logical_and(rim_high, gz == 0), pltpu.roll(given, 8 - comps, 0), 0.0)]
                    else:
                        ends = [ends[0] + jnp.where(rim_low, given, 0.0), ends[1] + jnp.where(rim_high, given, 0.0)]
                cut = [rest[:8] + ends[0], rest[8 : planes - 8], rest[planes - 8 :] + ends[1]]
                rest = jnp.concatenate(cut, axis=0)
                inner_side = jnp.logical_and(
                    jnp.logical_or(rest_id >= comps, open_low), jnp.logical_or(rest_id < planes - comps, open_high))
                for tile in range(tiles):
                    part = rest[:, tile * 128 : (tile + 1) * 128]
                    if tile == 0:
                        add = pltpu.roll(sides, 128 - 2 * line, 1)
                        part = part + jnp.where(jnp.logical_and(inner_side, tile_lane == 0), add, 0.0)
                    if tile == tiles - 1:
                        add = pltpu.roll(sides, 126 - 2 * line, 1)
                        part = part + jnp.where(jnp.logical_and(inner_side, tile_lane == 127), add, 0.0)
                    out_r[pl.ds(tile * rows + line, planes, stride=tiles * rows), :] = part

    row_id = lax.broadcasted_iota(jnp.int32, (rows, 128), 0)
    lane_id = lax.broadcasted_iota(jnp.int32, (rows, 128), 1)
    row_rim = jnp.logical_or(row_id == 0, row_id == rows - 1)

    def solution_tile(layer, c, tile):
        first = ((layer * comps + c) * tiles + tile) * rows
        return pl.ds(first, rows)

    def shares(layer, first):
        mat_id = mats[gz, layer]
        return [[coef[mat_id, first + i * comps + j] for j in three] for i in three]

    for layer in range(layers) if nz == 2 else range(1, layers - 1):
        mat = [shares(layer, which * comps * comps) for which in range(3)]
        for tile in range(tiles):
            here, side, vert = [], [], []
            for c in three:
                x = out_u[solution_tile(layer, c, tile), :]
                west = out_u[solution_tile(layer, c, tile - 1), :] if tile else x
                east = out_u[solution_tile(layer, c, tile + 1), :] if tile < tiles - 1 else x
                beside = jnp.where(lane_id == 127, west, x), jnp.where(lane_id == 0, east, x)
                around = pltpu.roll(beside[0], 1, 1) + pltpu.roll(beside[1], 127, 1)
                here.append(x)
                side.append(around + (pltpu.roll(x, 1, 0) + pltpu.roll(x, rows - 1, 0)))
                near = [out_u[solution_tile(z, c, tile), :] for z in (layer - 1, layer + 1) if 0 <= z < layers]
                vert.append(total(near))
            a, b, d = (times(mat[which], vec) for which, vec in enumerate((here, side, vert)))
            rim = row_rim
            if layer in (0, layers - 1):
                rim = jnp.logical_or(rim, jnp.logical_not(open_high if layer else open_low))
            if tile == 0:
                rim = jnp.logical_or(rim, lane_id == 0)
            if tile == tiles - 1:
                rim = jnp.logical_or(rim, lane_id == 127)
            for c in three:
                spot = solution_tile(layer, c, tile)
                first = ((layer * comps + c) * tiles + tile) * rows
                value = load[first : first + rows, :] - (a[c] - b[c] - d[c])
                out_r[spot, :] = jnp.where(rim, out_r[spot, :], value)
    for cond, copy in pending:
        if cond is True:
            copy.wait_send()
        else:
            @pl.when(cond)
            def _(copy=copy):
                copy.wait_send()


def put(from_u, from_r, to_u, to_r, sem):
    copies = [pltpu.make_async_copy(src, dst, sem.at[i]) for i, (src, dst) in enumerate(((from_u, to_u), (from_r, to_r)))]
    for copy in copies:
        copy.start()
    for copy in copies:
        copy.wait()


def solution(mesh):
    sizes = tuple(mesh.shape[name] for name in ("gz", "gy", "gx"))
    nz = sizes[0]

    def on_device(right_side, start_field, layer_material, stiffness, line_factors):
        dims = right_side.shape
        layers, comps, rows, lanes = dims
        planes = layers * comps
        deep = nz * layers
        half_group = -(-planes // 32) * 32
        depth = POWERS * 2 * half_group
        packed = -(-2 * rows * SLOT // 128) * 128
        f32 = jnp.float32
        vmem = pl.BlockSpec(memory_space=pltpu.VMEM)
        dma = pltpu.SemaphoreType.DMA
        others = max(nz - 1, 1)
        symbol = pltpu.VMEM((deep * comps, 8, 128), f32)
        tables = (3, comps, comps, stiffness.shape[0])
        flat = (planes * rows * lanes // 128, 128)
        scratch = [pltpu.SMEM((layers,), jnp.int32)]
        scratch += [pltpu.SMEM(tables, f32)] * 2
        scratch += [pltpu.VMEM(flat, f32)] * 2
        scratch += [pltpu.VMEM((tables[3], 2 * 3 * comps * comps, 8, 128), f32), dma((5,))]
        scratch += [pltpu.SMEM((nz, layers), jnp.int32)]
        scratch += [pltpu.VMEM((rows, planes, lanes), f32)] * 2
        scratch += [pltpu.VMEM((n, planes, lanes), f32) for n in (REACH, REACH - 1, REACH, REACH - 1)]
        scratch += [
            pltpu.VMEM((2, planes, packed), f32),
            pltpu.VMEM((3, 2, planes, packed), f32),
            pltpu.VMEM((REACH, rows + 2 * REACH, planes, lanes + 128), f32),
            pltpu.VMEM((REACH - 1, rows + 2 * REACH - 2, planes, lanes + 128), f32),
            pltpu.VMEM((3, planes, lanes + 128), f32),
        ]
        scratch += [symbol] * 6
        scratch += [
            pltpu.VMEM((nz * 2 * planes * 8, 128), f32),
            pltpu.VMEM((3 * nz * 2 * planes, depth), jnp.bfloat16),
            pltpu.VMEM((3, rows, depth, lanes), jnp.bfloat16),
            pltpu.VMEM((rows, 2 * planes, lanes), f32),
            pltpu.VMEM((others, rows, 2 * planes, lanes), f32),
            pltpu.VMEM((others, rows, 2 * planes, lanes), f32),
        ]
        scratch += [pltpu.VMEM((others, rows // 2, 2, 8, lanes), f32)] * 2 + [pltpu.VMEM((others, planes, 128), f32)] * 2
        scratch += [dma((nz,))] * 2 + [dma((2, REACH, 2))] * 2 + [dma((2,))] * 4 + [dma((others, rows))] * 2 + [dma((others, rows // 2, 2))] * 2 + [dma((others,))] * 2
        tiled = (layers, comps, rows, lanes // 128, 128)

        def flatten(x):
            return x.reshape(tiled).transpose(0, 1, 3, 2, 4).reshape(-1, 128)

        def unflatten(x):
            split = x.reshape(layers, comps, lanes // 128, rows, 128)
            return split.transpose(0, 1, 3, 2, 4).reshape(dims)

        out = jax.ShapeDtypeStruct(flat, f32)
        given = (layer_material, stiffness.transpose(1, 2, 3, 0), line_factors.transpose(1, 2, 3, 0),
                 flatten(right_side), flatten(start_field))
        given = [pltpu.with_memory_space_constraint(x, pltpu.HBM) for x in given]
        outs = pl.pallas_call(
            functools.partial(kernel, sizes, dims),
            out_shape=(out, out),
            in_specs=[pl.BlockSpec(memory_space=pltpu.HBM)] * 5,
            out_specs=(vmem, vmem),
            scratch_shapes=scratch,
            compiler_params=pltpu.CompilerParams(
                collective_id=0, has_side_effects=True, vmem_limit_bytes=VMEM_LIMIT),
        )(*given)
        outs = pl.pallas_call(
            put,
            out_shape=(out, out),
            in_specs=[vmem, vmem],
            out_specs=(pl.BlockSpec(memory_space=pltpu.HBM),) * 2,
            scratch_shapes=[dma((2,))],
            compiler_params=pltpu.CompilerParams(vmem_limit_bytes=4 * 1024 * 1024),
        )(*outs)
        return tuple(unflatten(o) for o in outs)

    return jax.shard_map(
        on_device,
        mesh=mesh,
        in_specs=(P("gz", None, "gy", "gx"), P("gz", None, "gy", "gx"), P("gz"), P(), P()),
        out_specs=(P("gz", None, "gy", "gx"), P("gz", None, "gy", "gx")),
        check_vma=False,
    )


VMEM_LIMIT = 40 * 1024 * 1024
```
